128 devices in a mesh: row: 16 (over x_hi, z, core), col: 8 (over x_lo, y).
Axes of the slice: x: 4 (x_hi: 2, x_lo: 2; x = x_hi * 2 + x_lo), y: 4, z: 4, core: 2. Of those that a mesh axis runs over, the one named last changes fastest.
Arguments:
- local_inverse: float32 [1024, 512, 512], P(('row', 'col')), may hold values from -1 to 3.5, as said below
- coupling: float32 [1024, 512, 1024], P(('row', 'col')), may hold values from -0.03125 to 0.03125
- local_rhs: float32 [1024, 512], P(('row', 'col')), may hold values from -6 to 6
- members: int32 [1024, 8], P(('row', 'col')), may hold values from 0 to 15, all different within a row
- shared_matrix: float32 [2048, 2048], P('row', 'col'), may hold values from -2 to 66, as said below
- shared_rhs: float32 [2048], P('row'), may hold values from -6 to 6
- prior_solution: float32 [2048], P('row'), may hold values from -6 to 6
- preconditioner: float32 [2048], P('row'), may hold values from 0.008 to 0.02
Outputs:
- reduced_matrix: float32 [2048, 2048], P('row', 'col')
- reduced_rhs: float32 [2048], P('row')
- solution: float32 [2048], P('row')
The draws below stay inside these ranges and needn't reach their ends.
Inputs may be any that keep to these rules, and one draw needn't show every extreme that they name: `members`: each week names 8 different station blocks. `local_inverse`: symmetric for every week. `shared_matrix`: symmetric.
All inputs are finite; a program needn't handle non-finite values.
Results may differ from the reference program's by a relative error of at most 0.00016.
Values sent between devices are 32-bit elements; how exact they have to be, the bound alone decides.
A program may use at most 256 MiB of HBM per device.

```python
import math
import jax
import jax.numpy as jnp
from jax import lax

LOCAL = 512
BLOCK = 128
BLOCKS = 16
TOUCHED = 8
ITERS = 2
WEEKS = 1024
SHARED = 2048


def draw_local_inverse(key, part):
    first, second = jax.random.split(jax.random.fold_in(key, 11))
    diagonal = jax.random.uniform(first, (WEEKS, LOCAL), jnp.float32, 1.0, 2.0)
    noise = jax.random.truncated_normal(second, -4.0, 4.0, (WEEKS, LOCAL, LOCAL), jnp.float32)
    spread = 0.4 / math.sqrt(2.0 * LOCAL)
    symmetric = (noise + jnp.swapaxes(noise, 1, 2)) * spread
    return symmetric + diagonal[:, :, None] * jnp.eye(LOCAL, dtype=jnp.float32)[None, :, :]


def draw_shared_matrix(key, part):
    first, second = jax.random.split(jax.random.fold_in(key, 23))
    diagonal = jax.random.uniform(first, (SHARED,), jnp.float32, 45.0, 60.0)
    noise = jax.random.truncated_normal(second, -4.0, 4.0, (SHARED, SHARED), jnp.float32)
    spread = 2.2 / math.sqrt(2.0 * SHARED)
    symmetric = (noise + noise.T) * spread
    return symmetric + jnp.diag(diagonal)


def levels(stream_key, shape, cuts, least, largest):
    level, own = 1.0, jax.random.fold_in(stream_key, 6)
    for dim, shards_of in cuts:
        heights = jnp.exp(jax.random.uniform(jax.random.fold_in(own, dim), (shards_of,), jnp.float32, least / len(cuts), largest / len(cuts)))
        level = level * jnp.repeat(heights, shape[dim] // shards_of).reshape([-1 if axis == dim else 1 for axis in range(len(shape))])
    return level


def different_ones(stream_key, rows, amount, top, lift):
    sequence = jax.random.permutation(jax.random.fold_in(stream_key, 1), amount)
    pull = sequence
    for power in range(3):
        pull = pull * pull // amount
    pull = pull * lift // amount
    tickets = jax.random.randint(jax.random.fold_in(stream_key, 2), (rows, amount), 0, 4096) + pull
    sure = jax.random.permutation(jax.random.fold_in(stream_key, 3), rows)[jnp.arange(amount) % rows]
    tickets = jnp.where(jnp.arange(rows)[:, None] == sure[None, :], 1 << 14, tickets)
    priority = tickets * amount + jnp.arange(amount)
    return lax.top_k(priority.astype(jnp.int32), top)[1].astype(jnp.int32)


def centred(stream_key, shape, scale, most, shards=(), held_as=jnp.bfloat16):
    entries = scale * jax.random.normal(stream_key, shape, jnp.float32)
    if shards:
        entries = entries * levels(stream_key, shape, shards, -0.22, 0.18)
    return jnp.clip(entries, -most, most).astype(held_as)


def setup_inputs(seed: int = 0) -> dict:
    keys = jax.random.split(jax.random.key(seed), 9)
    return {
        "local_inverse": draw_local_inverse(jax.random.fold_in(keys[8], 71), 0),
        "coupling": centred(keys[1], (WEEKS, LOCAL, TOUCHED * BLOCK), (LOCAL * WEEKS // 16) ** -0.5, 0.03125, ((0, 128),), jnp.float32),
        "local_rhs": centred(keys[2], (WEEKS, LOCAL), 1.0, 6.0, ((0, 128),), jnp.float32),
        "members": different_ones(keys[3], WEEKS, BLOCKS, TOUCHED, 4096),
        "shared_matrix": draw_shared_matrix(jax.random.fold_in(keys[8], 71), 0),
        "shared_rhs": centred(keys[5], (SHARED,), 1.0, 6.0, ((0, 16),), jnp.float32),
        "prior_solution": centred(keys[6], (SHARED,), 1.0, 6.0, ((0, 16),), jnp.float32),
        "preconditioner": jnp.clip(jnp.exp(math.log(0.02) - 0.91629066 * jax.random.uniform(keys[7], (SHARED,), jnp.float32) ** levels(keys[7], (SHARED,), ((0, 16),), -0.2, 0.2)), 0.008, 0.02),
    }


def eliminate(accumulated, items):
    grid_sum, rhs_sum = accumulated
    inverse, coupling_week, rhs_week, blocks = items
    mapped = jnp.dot(inverse, coupling_week, precision=lax.Precision.HIGHEST, preferred_element_type=jnp.float32)
    contribution = jnp.dot(coupling_week.T, mapped, precision=lax.Precision.HIGHEST, preferred_element_type=jnp.float32)
    pushed = jnp.dot(rhs_week, mapped, precision=lax.Precision.HIGHEST, preferred_element_type=jnp.float32)
    tile_grid = contribution.reshape(TOUCHED, BLOCK, TOUCHED, BLOCK).transpose(0, 2, 1, 3)
    grid_sum = grid_sum.at[blocks[:, None], blocks[None, :]].add(tile_grid)
    rhs_sum = rhs_sum.at[blocks].add(pushed.reshape(TOUCHED, BLOCK))
    return (grid_sum, rhs_sum), None


def reference(local_inverse, coupling, local_rhs, members, shared_matrix, shared_rhs, prior_solution, preconditioner):
    start_grid = jnp.zeros((BLOCKS, BLOCKS, BLOCK, BLOCK), jnp.float32)
    start_rhs = jnp.zeros((BLOCKS, BLOCK), jnp.float32)
    (grid_sum, rhs_sum), unused = lax.scan(eliminate, (start_grid, start_rhs), (local_inverse, coupling, local_rhs, members.astype(jnp.int32)))
    eliminated = grid_sum.transpose(0, 2, 1, 3).reshape(SHARED, SHARED)
    reduced_matrix = shared_matrix - eliminated
    reduced_rhs = shared_rhs - rhs_sum.reshape(SHARED)
    solution = prior_solution
    for iteration in range(ITERS):
        product = jnp.dot(reduced_matrix, solution, precision=lax.Precision.HIGHEST, preferred_element_type=jnp.float32)
        solution = solution + preconditioner * (reduced_rhs - product)
    return (reduced_matrix, reduced_rhs, solution)
```

```python
import functools

import jax
import jax.numpy as jnp
from jax import lax
from jax.experimental import pallas as pl
from jax.experimental.pallas import tpu as pltpu
from jax.sharding import PartitionSpec as P

BLOCK = 128
BLOCKS = 16
TOUCHED = 8
LOCAL = 512
PASSES = 3
HEAD = 16
COLORS = 3
PIECES = 6
GRID = COLORS * 2 * 64 * PIECES
MESH = pl.DeviceIdType.MESH
f32 = jnp.float32
bf16 = jnp.bfloat16


def split(value):
    high = value.astype(bf16)
    return high, (value - high.astype(f32)).astype(bf16)


def product(left, right):
    total = jnp.dot(left[0], right[0], preferred_element_type=f32)
    if PASSES == 3:
        total += jnp.dot(left[1], right[0], preferred_element_type=f32)
        total += jnp.dot(left[0], right[1], preferred_element_type=f32)
    return total


def piece_base(block):
    core, z = block % 2, (block // 2) % 4
    return core * 384 + (block // 8) * 192 + z * PIECES


def eliminate(
    members, inverse, coupling, rhs, summed, turned_h, turned_l, held_h, held_l, mapped_h, mapped_l
):
    week = pl.program_id(0)

    @pl.when(week == 0)
    def clear():
        @pl.loop(0, GRID // 16)
        def step(index):
            summed[pl.ds(index * 16, 16)] = jnp.zeros((16, 8, BLOCK), f32)

    blocks = [members[week, k] for k in range(TOUCHED)]
    ranks = [
        sum((blocks[j] < blocks[k]).astype(jnp.int32) for j in range(TOUCHED) if j != k)
        for k in range(TOUCHED)
    ]
    place, held = [], []
    for a in range(TOUCHED):
        here = [(ranks[k] == a).astype(jnp.int32) for k in range(TOUCHED)]
        place.append(sum(here[k] * k for k in range(1, TOUCHED)))
        held.append(sum(here[k] * blocks[k] for k in range(TOUCHED)))
    for a in range(TOUCHED):
        columns = coupling[0, :, pl.ds(pl.multiple_of(place[a] * BLOCK, BLOCK), BLOCK)]
        at = slice(a * BLOCK, (a + 1) * BLOCK)
        held_h[:, at], low = split(columns)
        if PASSES == 3:
            held_l[:, at] = low
        at = slice(HEAD + a * BLOCK, HEAD + (a + 1) * BLOCK)
        turned_h[at, :], low = split(columns.T)
        if PASSES == 3:
            turned_l[at, :] = low
    row = lax.broadcasted_iota(jnp.int32, (HEAD, LOCAL), 0)
    first = jnp.where(row == 0, jnp.broadcast_to(rhs[0], (HEAD, LOCAL)), 0.0)
    turned_h[0:HEAD, :], low = split(first)
    if PASSES == 3:
        turned_l[0:HEAD, :] = low
    for n in range(2):
        at = slice(n * 256, n * 256 + 256)
        part = product((turned_h[...], turned_l[...]), split(inverse[0, :, at]))
        mapped_h[:, at], low = split(part)
        if PASSES == 3:
            mapped_l[:, at] = low
    for n in range(4):
        at = slice(n * 256, n * 256 + 256)
        rows = slice(0, HEAD + (n + 1) * 256)
        part = product((mapped_h[rows, :], mapped_l[rows, :]), (held_h[:, at], held_l[:, at]))
        for b in (2 * n, 2 * n + 1):
            lanes = slice((b - 2 * n) * BLOCK, (b - 2 * n + 1) * BLOCK)
            index = 2 * 768 + piece_base(held[b]) + (held[b] // 8) * 96
            index += ((held[b] // 2) % 4) * 24 + PIECES - 1
            summed[index] = summed[index] + part[0:8, lanes]
            for a in range(b + 1):
                low_half = held[a] < 8
                group = jnp.where(low_half, held[a], 15 - held[a])
                piece = jnp.where(low_half, held[b] - held[a], held[b] + 1)
                start = (piece // PIECES) * 768 + piece % PIECES
                tile = part[HEAD + a * BLOCK : HEAD + (a + 1) * BLOCK, lanes].reshape(16, 8, BLOCK)
                places = []
                for s in range(16):
                    base = start + piece_base(group if s < 8 else 15 - group)
                    places.append(base + (s % 8 // 4) * 96 + (s % 4) * 24)
                new = [summed[places[s]] + tile[s] for s in range(16)]
                for s in range(16):
                    summed[places[s]] = new[s]


def device(x, y, z, core):
    return {"row": (x // 2) * 8 + z * 2 + core, "col": (x % 2) * 4 + y}


def combine(
    data, matrix, rhs, prior, weight,
    out_matrix, out_rhs, out_solution,
    own, other, relay1, final1, sum1, relay2, final2, sum2, relay3, final3, sum3,
    land, block_out, blocks_in, partial1, partial2, row1, column1, row2,
    load_sem, pair_send, pair_recv, ring_send, ring_recv,
    tile_send, tile_recv, block_send, block_recv,
    one_send, one_recv, column_send, column_recv, two_send, two_recv,
):
    r, c = lax.axis_index("row"), lax.axis_index("col")
    core, z = r % 2, (r // 2) % 4
    x, y = (r // 8) * 2 + c // 4, c % 4
    me = (x, y, z)

    def neighbour(axis, step):
        at = list(me)
        at[axis] = (me[axis] + step) % 4
        return device(*at, core)

    barrier = pltpu.get_barrier_semaphore()
    partner = {"row": r + 1 - 2 * core, "col": c}
    greeted = [partner] + [neighbour(axis, step) for axis in range(3) for step in (1, 3)]
    for target in greeted:
        pl.semaphore_signal(barrier, inc=1, device_id=target, device_id_type=MESH)

    def cut(ref, lead, position, index, half=None):
        picks = [slice(None)] * position + [index]
        if half is not None:
            size = ref.shape[len(lead)] // 2 if position else ref.shape[len(lead) + 1] // 2
            keep = pl.ds(half * size, size)
            if position:
                picks[0] = keep
            else:
                picks.append(keep)
        return ref.at[(*lead, *picks)]

    steps = (2, 1, 3, 0)

    def loads(color, j):
        at = (me[color] + j) % 4
        src = cut(data, (color, core), color, at)
        return pltpu.make_async_copy(src, cut(own, (color,), color, at), load_sem.at[color, j])

    def pairs(color, j):
        at = (me[color] + j) % 4
        return pltpu.make_async_remote_copy(
            src_ref=cut(data, (color, 1 - core), color, at),
            dst_ref=cut(other, (color,), color, at),
            send_sem=pair_send.at[color, j],
            recv_sem=pair_recv.at[color, j],
            device_id=partner,
            device_id_type=MESH,
        )

    for j in steps:
        for color in range(COLORS):
            loads(color, j).start()
    pl.semaphore_wait(barrier, len(greeted))
    for j in steps:
        for color in range(COLORS):
            pairs(color, j).start()

    def add(target, *terms):
        value = target[...]
        for term in terms:
            value = value + term[...]
        target[...] = value

    def arrived(color, j):
        at = (me[color] + j) % 4
        loads(color, j).wait()
        pairs(color, j).wait_recv()
        add(cut(own, (color,), color, at), cut(other, (color,), color, at))

    axes = ((0, 1, 2), (1, 2, 0), (2, 0, 1))
    spots = ((0, 0), (1, 1), (2, 0))
    waiting = []

    def phase(number, source, relay, final, result, prepare):
        def hop(color, slot, step, src, dst):
            copy = pltpu.make_async_remote_copy(
                src_ref=src,
                dst_ref=dst,
                send_sem=ring_send.at[number, color, slot],
                recv_sem=ring_recv.at[number, color, slot],
                device_id=neighbour(axes[color][number], step),
                device_id_type=MESH,
            )
            return copy

        def source_cut(color, step, half):
            at = (me[axes[color][number]] + step) % 4
            if number == 2:
                return source.at[color, at] if half is None else source.at[color, at, pl.ds(half * 24, 24)]
            return cut(source, (color,), spots[color][number], at, half)

        def landing(ref, color, side, half):
            if half is None:
                return ref.at[color, side]
            size = ref.shape[2] // 2
            return ref.at[color, side, pl.ds(half * size, size)]

        def away(color, side):
            return hop(color, side, (1, 3)[side], source_cut(color, 2, side), relay.at[color, side])

        def near(color, side, half):
            step = (1, 3)[side]
            return hop(
                color, 2 + 2 * side + half, step,
                source_cut(color, step, half), landing(final, color, side, half),
            )

        for color in range(COLORS):
            prepare(color, 2)
            for side in range(2):
                away(color, side).start()
        for color in range(COLORS):
            for side in range(2):
                prepare(color, (1, 3)[side])
                near(color, side, 1 - side).start()
        for color in range(COLORS):
            for side in range(2):
                away(color, side).wait_recv()
                add(source_cut(color, (1, 3)[side], side), relay.at[color, side])
                near(color, side, side).start()
        for color in range(COLORS):
            prepare(color, 0)
            for side in range(2):
                for half in range(2):
                    near(color, side, half).wait_recv()
            mine = source_cut(color, 0, None)
            result[color] = mine[...] + final[color, 0] + final[color, 1]
        for color in range(COLORS):
            for side in range(2):
                waiting.append(away(color, side))
                for half in range(2):
                    waiting.append(near(color, side, half))

    def nothing(color, j):
        pass

    phase(0, own, relay1, final1, sum1, arrived)
    phase(1, sum1, relay2, final2, sum2, nothing)
    phase(2, sum2, relay3, final3, sum3, nothing)

    low_half = r < 8
    group = jnp.where(low_half, r, 15 - r)
    strip = jnp.where(low_half, c, c + 8)

    def piece(t):
        return sum3.at[t // PIECES, pl.ds((t % PIECES) * 8, 8)]

    def tile_copy(t, mirrored):
        first = t < 16 - group
        i = jnp.where(first, group, 15 - group)
        j = jnp.where(first, group + t, t - 1)
        row, column = (j, i) if mirrored else (i, j)
        copy = pltpu.make_async_remote_copy(
            src_ref=piece(t),
            dst_ref=land.at[column % 2, strip],
            send_sem=tile_send.at[t, int(mirrored)],
            recv_sem=tile_recv.at[column % 2, strip],
            device_id={"row": row, "col": column // 2},
            device_id_type=MESH,
        )
        mine = (row == r) & (column // 2 == c)
        wanted = (i != j) if mirrored else None
        return copy, mine, wanted, column % 2

    holder = c == r // 2

    def to_column(d):
        return pltpu.make_async_remote_copy(
            src_ref=block_out,
            dst_ref=blocks_in.at[1 + r % 2],
            send_sem=block_send.at[d],
            recv_sem=block_recv.at[1 + r % 2],
            device_id={"row": (r + d) % 16, "col": c},
            device_id_type=MESH,
        )

    def to_row(d):
        return pltpu.make_async_remote_copy(
            src_ref=block_out,
            dst_ref=blocks_in.at[0],
            send_sem=block_send.at[15 + d],
            recv_sem=block_recv.at[0],
            device_id={"row": r, "col": (c + d) % 8},
            device_id_type=MESH,
        )

    @pl.when(holder)
    def hand_out():
        reduced = rhs[...] - sum3[2, 40:41, :]
        row = lax.broadcasted_iota(jnp.int32, (8, BLOCK), 0)
        value = jnp.where(row == 0, reduced, jnp.where(row == 1, prior[...], weight[...]))
        block_out[...] = value
        blocks_in[0] = value
        blocks_in[1 + r % 2] = value
        for d in range(1, 16):
            to_column(d).start()
        for d in range(1, 8):
            to_row(d).start()

    for t in range(17):
        for mirrored in (False, True):
            copy, mine, wanted, side = tile_copy(t, mirrored)
            away = jnp.logical_not(mine)
            if wanted is not None:
                mine, away = mine & wanted, away & wanted

            @pl.when(away)
            def send():
                copy.start()

            @pl.when(mine)
            def keep():
                land[side, strip] = piece(t)[...]

    def receive(buffer, semaphore):
        pltpu.make_async_remote_copy(
            src_ref=buffer,
            dst_ref=buffer,
            send_sem=semaphore,
            recv_sem=semaphore,
            device_id=partner,
            device_id_type=MESH,
        ).wait_recv()

    for side in range(2):
        column = 2 * c + side
        low = jnp.minimum(r, column)
        owner = jnp.where(low < 8, low, 15 - low)
        for s in range(16):
            row = owner if s < 8 else 15 - owner

            @pl.when(jnp.logical_not((row == r) & (c == s % 8)))
            def wait():
                receive(land.at[side, s], tile_recv.at[side, s])

    tiles = []
    for side in range(2):
        found = land[side].reshape(BLOCK, BLOCK)
        found = jnp.where(r > 2 * c + side, found.T, found)
        lanes = slice(side * BLOCK, (side + 1) * BLOCK)
        tile = matrix[:, lanes] - found
        out_matrix[:, lanes] = tile
        tiles.append(tile)

    @pl.when(jnp.logical_not(holder))
    def row_block():
        receive(blocks_in.at[0], block_recv.at[0])

    for side in range(2):

        @pl.when(r != 2 * c + side)
        def column_block():
            receive(blocks_in.at[1 + side], block_recv.at[1 + side])

    reduced = blocks_in[0, 0:1, :]
    out_rhs[...] = reduced

    def matvec(first, second):
        spread = tiles[0] * first + tiles[1] * second
        return jnp.broadcast_to(jnp.sum(spread.T, axis=0, keepdims=True), (8, BLOCK))

    def along_row(d, source, target, sends, recvs):
        return pltpu.make_async_remote_copy(
            src_ref=source,
            dst_ref=target.at[c],
            send_sem=sends.at[d],
            recv_sem=recvs.at[c],
            device_id={"row": r, "col": (c + d) % 8},
            device_id_type=MESH,
        )

    def along_column(d):
        return pltpu.make_async_remote_copy(
            src_ref=partial1,
            dst_ref=column1.at[r % 2, c],
            send_sem=column_send.at[d],
            recv_sem=column_recv.at[r % 2, c],
            device_id={"row": (r + d) % 16, "col": r // 2},
            device_id_type=MESH,
        )

    value = matvec(blocks_in[1, 1:2, :], blocks_in[2, 1:2, :])
    partial1[...] = value
    row1[c] = value
    for d in range(1, 16):
        along_column(d).start()

    @pl.when(jnp.logical_not(holder))
    def last_column():
        along_column(0).start()

    @pl.when(holder)
    def own_column():
        column1[r % 2, c] = value

    for d in range(1, 8):
        along_row(d, partial1, row1, one_send, one_recv).start()

    def gather_row(target, recvs):
        for s in range(8):

            @pl.when(c != s)
            def wait():
                receive(target.at[s], recvs.at[s])

    def total(ref):
        value = ref[0, 0:1, :]
        for s in range(1, 8):
            value = value + ref[s, 0:1, :]
        return value

    def updated(block, product):
        return block[1:2, :] + block[2:3, :] * (block[0:1, :] - product)

    for side in range(2):
        for s in range(8):

            @pl.when(jnp.logical_not((r == 2 * c + side) & (c == s)))
            def wait():
                receive(column1.at[side, s], column_recv.at[side, s])

    first = [updated(blocks_in[1 + side], total(column1.at[side])) for side in range(2)]
    value = matvec(*first)
    partial2[...] = value
    row2[c] = value
    for d in range(1, 8):
        along_row(d, partial2, row2, two_send, two_recv).start()
    gather_row(row1, one_recv)
    mine = updated(blocks_in[0], total(row1))
    gather_row(row2, two_recv)
    out_solution[...] = mine + weight[...] * (reduced - total(row2))

    for color in range(COLORS):
        for j in steps:
            pairs(color, j).wait_send()
    for copy in waiting:
        copy.wait_send()
    for t in range(17):
        for mirrored in (False, True):
            copy, mine, wanted, side = tile_copy(t, mirrored)
            away = jnp.logical_not(mine)
            if wanted is not None:
                away = away & wanted

            @pl.when(away)
            def sent():
                copy.wait_send()

    @pl.when(holder)
    def handed():
        for d in range(1, 16):
            to_column(d).wait_send()
        for d in range(1, 8):
            to_row(d).wait_send()

    for d in range(1, 16):
        along_column(d).wait_send()

    @pl.when(jnp.logical_not(holder))
    def last_sent():
        along_column(0).wait_send()

    for d in range(1, 8):
        along_row(d, partial1, row1, one_send, one_recv).wait_send()
        along_row(d, partial2, row2, two_send, two_recv).wait_send()


def partial_sum(local_inverse, coupling, local_rhs, members):
    weeks = local_inverse.shape[0]
    mapped = pltpu.VMEM((HEAD + TOUCHED * BLOCK, LOCAL), bf16)
    held = pltpu.VMEM((LOCAL, TOUCHED * BLOCK), bf16)
    return pl.pallas_call(
        eliminate,
        grid_spec=pltpu.PrefetchScalarGridSpec(
            num_scalar_prefetch=1,
            grid=(weeks,),
            in_specs=[
                pl.BlockSpec((1, LOCAL, LOCAL), lambda w, m: (w, 0, 0)),
                pl.BlockSpec((1, LOCAL, TOUCHED * BLOCK), lambda w, m: (w, 0, 0)),
                pl.BlockSpec((1, 1, LOCAL), lambda w, m: (w, 0, 0)),
            ],
            out_specs=pl.BlockSpec((GRID, 8, BLOCK), lambda w, m: (0, 0, 0)),
            scratch_shapes=[mapped, mapped, held, held, mapped, mapped],
        ),
        out_shape=jax.ShapeDtypeStruct((GRID, 8, BLOCK), f32),
        compiler_params=pltpu.CompilerParams(
            dimension_semantics=("arbitrary",), vmem_limit_bytes=60 * 2**20
        ),
        name="eliminate",
    )(members, local_inverse, coupling, local_rhs.reshape(weeks, 1, LOCAL))


def combined(summed, shared_matrix, shared_rhs, prior_solution, preconditioner):
    rows, columns = shared_matrix.shape
    vmem = pl.BlockSpec(memory_space=pltpu.VMEM)
    strip = PIECES * 8
    dma = pltpu.SemaphoreType.DMA

    def buffer(*shape):
        return pltpu.VMEM(shape, f32)

    return pl.pallas_call(
        combine,
        in_specs=[pl.BlockSpec(memory_space=pl.ANY)] + [vmem] * 4,
        out_specs=[vmem] * 3,
        out_shape=[
            jax.ShapeDtypeStruct((rows, columns), f32),
            jax.ShapeDtypeStruct((1, rows), f32),
            jax.ShapeDtypeStruct((1, rows), f32),
        ],
        scratch_shapes=[
            buffer(COLORS, 4, 4, 4, strip, BLOCK),
            buffer(COLORS, 4, 4, 4, strip, BLOCK),
            buffer(COLORS, 2, 2, 4, strip, BLOCK),
            buffer(COLORS, 2, 4, 4, strip, BLOCK),
            buffer(COLORS, 4, 4, strip, BLOCK),
            buffer(COLORS, 2, 2, strip, BLOCK),
            buffer(COLORS, 2, 4, strip, BLOCK),
            buffer(COLORS, 4, strip, BLOCK),
            buffer(COLORS, 2, strip // 2, BLOCK),
            buffer(COLORS, 2, strip, BLOCK),
            buffer(COLORS, strip, BLOCK),
            buffer(2, 16, 8, BLOCK),
            buffer(8, BLOCK),
            buffer(3, 8, BLOCK),
            buffer(8, BLOCK),
            buffer(8, BLOCK),
            buffer(8, 8, BLOCK),
            buffer(2, 8, 8, BLOCK),
            buffer(8, 8, BLOCK),
            dma((COLORS, 4)),
            dma((COLORS, 4)),
            dma((COLORS, 4)),
            dma((3, COLORS, 6)),
            dma((3, COLORS, 6)),
            dma((17, 2)),
            dma((2, 16)),
            dma((23,)),
            dma((3,)),
            dma((8,)),
            dma((8,)),
            dma((16,)),
            dma((2, 8)),
            dma((8,)),
            dma((8,)),
        ],
        compiler_params=pltpu.CompilerParams(
            collective_id=0, has_side_effects=True, vmem_limit_bytes=40 * 2**20
        ),
        name="combine",
    )(
        summed.reshape(COLORS, 2, 4, 4, 4, strip, BLOCK),
        shared_matrix,
        shared_rhs.reshape(1, rows),
        prior_solution.reshape(1, rows),
        preconditioner.reshape(1, rows),
    )


def local(
    local_inverse,
    coupling,
    local_rhs,
    members,
    shared_matrix,
    shared_rhs,
    prior_solution,
    preconditioner,
):
    summed = partial_sum(local_inverse, coupling, local_rhs, members)
    reduced_matrix, reduced_rhs, solution = combined(
        summed, shared_matrix, shared_rhs, prior_solution, preconditioner
    )
    return reduced_matrix, reduced_rhs.reshape(-1), solution.reshape(-1)


def solution(mesh):
    both = ("row", "col")
    placed = (
        P(both, None, None),
        P(both, None, None),
        P(both, None),
        P(both, None),
        P("row", "col"),
        P("row"),
        P("row"),
        P("row"),
    )
    return jax.shard_map(
        local,
        mesh=mesh,
        in_specs=placed,
        out_specs=(P("row", "col"), P("row"), P("row")),
        check_vma=False,
    )
```

```python
import functools

import jax
import jax.numpy as jnp
from jax import lax
from jax.experimental import pallas as pl
from jax.experimental.pallas import tpu as pltpu
from jax.sharding import PartitionSpec as P

BLOCK = 128
BLOCKS = 16
TOUCHED = 8
LOCAL = 512
PASSES = 3
HEAD = 16
COLORS = 3
PIECES = 6
GRID = COLORS * 2 * 64 * PIECES
MESH = pl.DeviceIdType.MESH
f32 = jnp.float32
bf16 = jnp.bfloat16


def split(value):
    high = value.astype(bf16)
    return high, (value - high.astype(f32)).astype(bf16)


def product(left, right):
    total = jnp.dot(left[0], right[0], preferred_element_type=f32)
    if PASSES == 3:
        total += jnp.dot(left[1], right[0], preferred_element_type=f32)
        total += jnp.dot(left[0], right[1], preferred_element_type=f32)
    return total


def piece_base(block):
    core, z = block % 2, (block // 2) % 4
    return core * 384 + (block // 8) * 192 + z * PIECES


def eliminate(
    members, inverse, coupling, rhs, summed,
    inverse_in, coupling_in, in_sem,
    turned, held, kept, mapped,
):
    weeks = inverse.shape[0]

    def fetch(week, slot):
        return (
            pltpu.make_async_copy(inverse.at[week], inverse_in[slot], in_sem.at[slot, 0]),
            pltpu.make_async_copy(coupling.at[week], coupling_in[slot], in_sem.at[slot, 1]),
        )

    def start(week, slot):
        for copy in fetch(week, slot):
            copy.start()

    def wait(week, slot):
        for copy in fetch(week, slot):
            copy.wait()

    def order(week):
        blocks = [members[week, k] for k in range(TOUCHED)]
        ranks = [
            sum((blocks[j] < blocks[k]).astype(jnp.int32) for j in range(TOUCHED) if j != k)
            for k in range(TOUCHED)
        ]
        place, sorted_blocks = [], []
        for a in range(TOUCHED):
            here = [(ranks[k] == a).astype(jnp.int32) for k in range(TOUCHED)]
            place.append(sum(here[k] * k for k in range(1, TOUCHED)))
            sorted_blocks.append(sum(here[k] * blocks[k] for k in range(TOUCHED)))
        return place, sorted_blocks

    def prepare(week, slot):
        place, _ = order(week)

        def columns_of(a):
            def work():
                columns = coupling_in[slot][:, pl.ds(pl.multiple_of(place[a] * BLOCK, BLOCK), BLOCK)]
                at = slice(a * BLOCK, (a + 1) * BLOCK)
                held[slot][0][:, at], held[slot][1][:, at] = split(columns)
                at = slice(HEAD + a * BLOCK, HEAD + (a + 1) * BLOCK)
                turned[slot][0][at, :], turned[slot][1][at, :] = split(columns.T)

            return work

        def inverse_part(n):
            def work():
                at = slice(n * 128, n * 128 + 128)
                kept[slot][0][at, :], kept[slot][1][at, :] = split(inverse_in[slot][at, :])

            return work

        def head():
            row = lax.broadcasted_iota(jnp.int32, (HEAD, LOCAL), 0)
            first = jnp.where(row == 0, jnp.broadcast_to(rhs[pl.ds(week, 1), :], (HEAD, LOCAL)), 0.0)
            turned[slot][0][0:HEAD, :], turned[slot][1][0:HEAD, :] = split(first)

        return [head] + [inverse_part(n) for n in range(4)] + [columns_of(a) for a in range(TOUCHED)]

    def multiply(week, slot):
        _, blocks = order(week)

        def map_part(n, rows):
            def work():
                at = slice(n * 256, n * 256 + 256)
                part = product(
                    (turned[slot][0][rows, :], turned[slot][1][rows, :]),
                    (kept[slot][0][:, at], kept[slot][1][:, at]),
                )
                mapped[0][rows, at], mapped[1][rows, at] = split(part)

            return work

        def add_tiles(n, part, offset, places):
            for b in (2 * n, 2 * n + 1):
                lanes = slice((b - 2 * n) * BLOCK, (b - 2 * n + 1) * BLOCK)
                for a in places:
                    if a == -1:
                        index = 2 * 768 + piece_base(blocks[b]) + (blocks[b] // 8) * 96
                        index += ((blocks[b] // 2) % 4) * 24 + PIECES - 1
                        summed[index] = summed[index] + part[0:8, lanes]
                    elif a <= b:
                        low_half = blocks[a] < 8
                        group = jnp.where(low_half, blocks[a], 15 - blocks[a])
                        piece = jnp.where(low_half, blocks[b] - blocks[a], blocks[b] + 1)
                        first = (piece // PIECES) * 768 + piece % PIECES
                        top = HEAD + a * BLOCK - offset
                        tile = part[top : top + BLOCK, lanes].reshape(16, 8, BLOCK)
                        spots = []
                        for s in range(16):
                            base = first + piece_base(group if s < 8 else 15 - group)
                            spots.append(base + (s % 8 // 4) * 96 + (s % 4) * 24)
                        new = [summed[spots[s]] + tile[s] for s in range(16)]
                        for s in range(16):
                            summed[spots[s]] = new[s]

        def pair_part(n, m):
            def work():
                low = 0 if m == 0 else HEAD + m * 256
                rows = slice(low, HEAD + (m + 1) * 256)
                at = slice(n * 256, n * 256 + 256)
                part = product(
                    (mapped[0][rows, :], mapped[1][rows, :]),
                    (held[slot][0][:, at], held[slot][1][:, at]),
                )
                add_tiles(n, part, low, ([-1] if m == 0 else []) + [2 * m, 2 * m + 1])

            return work

        cuts = [slice(0, HEAD + 256)] + [slice(HEAD + k * 256, HEAD + k * 256 + 256) for k in (1, 2, 3)]
        first = [map_part(n, rows) for rows in cuts for n in range(2)]
        return first + [pair_part(n, m) for n in range(4) for m in range(n + 1)]

    def half_step(week, slot):
        other = 1 - slot

        @pl.when(week + 1 < weeks)
        def arrive():
            wait(week + 1, other)

        @pl.when(week + 2 < weeks)
        def ahead():
            start(week + 2, slot)

        work = multiply(week, slot)
        more = prepare(jnp.minimum(week + 1, weeks - 1), other)
        for index, item in enumerate(work):
            item()
            if index < len(more):
                more[index]()

    start(0, 0)
    start(1, 1)

    @pl.loop(0, GRID // 16)
    def clear(index):
        summed[pl.ds(index * 16, 16)] = jnp.zeros((16, 8, BLOCK), f32)

    wait(0, 0)
    for item in prepare(0, 0):
        item()

    @pl.loop(0, weeks // 2)
    def step(index):
        half_step(2 * index, 0)
        half_step(2 * index + 1, 1)


def device(x, y, z, core):
    return {"row": (x // 2) * 8 + z * 2 + core, "col": (x % 2) * 4 + y}


def combine(
    data, matrix, rhs, prior, weight,
    out_matrix, out_rhs, out_solution,
    own, other, relay1, final1, sum1, relay2, final2, sum2, final3, sum3,
    land, block_out, blocks_in, partial1, partial2, row1, column1, row2,
    load_sem, pair_send, pair_recv, ring_send, ring_recv,
    tile_send, tile_recv, block_send, block_recv,
    one_send, one_recv, column_send, column_recv, two_send, two_recv,
):
    r, c = lax.axis_index("row"), lax.axis_index("col")
    core, z = r % 2, (r // 2) % 4
    x, y = (r // 8) * 2 + c // 4, c % 4
    me = (x, y, z)

    def neighbour(axis, step):
        at = list(me)
        at[axis] = (me[axis] + step) % 4
        return device(*at, core)

    barrier = pltpu.get_barrier_semaphore()
    partner = {"row": r + 1 - 2 * core, "col": c}
    greeted = [partner] + [neighbour(axis, step) for axis in range(3) for step in (1, 3)]
    for target in greeted:
        pl.semaphore_signal(barrier, inc=1, device_id=target, device_id_type=MESH)

    strip_rows = [pl.ds(24 * part, 24) for part in range(2)]

    def cut(ref, lead, dims, position, index, part, half=None):
        picks = [slice(None)] * dims
        picks[position] = index
        if half is not None:
            picks[0 if position else 1] = pl.ds(2 * half, 2)
        return ref.at[(*lead, *picks, strip_rows[part])]

    def loads(color, j, part):
        at = (me[color] + j) % 4
        src = cut(data, (color, core), 3, color, at, part)
        dst = cut(own, (color,), 3, color, at, part)
        return pltpu.make_async_copy(src, dst, load_sem.at[part, color, j])

    def pairs(color, j, part):
        at = (me[color] + j) % 4
        return pltpu.make_async_remote_copy(
            src_ref=cut(data, (color, 1 - core), 3, color, at, part),
            dst_ref=cut(other, (color,), 3, color, at, part),
            send_sem=pair_send.at[part, color, j],
            recv_sem=pair_recv.at[part, color, j],
            device_id=partner,
            device_id_type=MESH,
        )

    everything = [(2, 0), (1, 0), (3, 0), (2, 1), (0, 0), (1, 1), (3, 1), (0, 1)]
    for j, part in everything:
        for color in range(COLORS):
            loads(color, j, part).start()
    pl.semaphore_wait(barrier, len(greeted))
    for j, part in everything:
        for color in range(COLORS):
            pairs(color, j, part).start()

    def add(target, *terms):
        value = target[...]
        for term in terms:
            value = value + term[...]
        target[...] = value

    def arrived(color, j, part):
        at = (me[color] + j) % 4
        loads(color, j, part).wait()
        pairs(color, j, part).wait_recv()
        add(cut(own, (color,), 3, color, at, part), cut(other, (color,), 3, color, at, part))

    axes = ((0, 1, 2), (1, 2, 0), (2, 0, 1))
    spots = ((0, 0), (1, 1), (2, 0))
    waiting = []

    def hop(number, color, slot, step, part, src, dst):
        return pltpu.make_async_remote_copy(
            src_ref=src,
            dst_ref=dst,
            send_sem=ring_send.at[part, number, color, slot],
            recv_sem=ring_recv.at[part, number, color, slot],
            device_id=neighbour(axes[color][number], step),
            device_id_type=MESH,
        )

    def ring(number, source, relay, final, result, prepare):
        dims = 3 - number

        def source_cut(color, step, part, half=None):
            at = (me[axes[color][number]] + step) % 4
            return cut(source, (color,), dims, spots[color][number], at, part, half)

        def landing(color, side, part, half=None):
            picks = [slice(None)] * (dims - 1)
            if half is not None:
                picks[0] = pl.ds(2 * half, 2)
            return final.at[(color, side, *picks, strip_rows[part])]

        def relayed(color, side, part):
            return relay.at[(color, side, *[slice(None)] * (dims - 1), strip_rows[part])]

        def away(color, side, part):
            src = source_cut(color, 2, part, side)
            return hop(number, color, side, (1, 3)[side], part, src, relayed(color, side, part))

        def near(color, side, part, half):
            step = (1, 3)[side]
            src = source_cut(color, step, part, half)
            dst = landing(color, side, part, half)
            return hop(number, color, 2 + 2 * side + half, step, part, src, dst)

        def far(part):
            for color in range(COLORS):
                prepare(color, 2, part)
                for side in range(2):
                    away(color, side, part).start()
                    waiting.append(away(color, side, part))

        def close(part):
            for color in range(COLORS):
                for side in range(2):
                    prepare(color, (1, 3)[side], part)
                    near(color, side, part, 1 - side).start()

        def pass_on(part):
            for color in range(COLORS):
                for side in range(2):
                    away(color, side, part).wait_recv()
                    add(source_cut(color, (1, 3)[side], part, side), relayed(color, side, part))
                    near(color, side, part, side).start()

        def finish(part):
            for color in range(COLORS):
                prepare(color, 0, part)
                for side in range(2):
                    for half in range(2):
                        near(color, side, part, half).wait_recv()
                        waiting.append(near(color, side, part, half))
                total = source_cut(color, 0, part)[...] + landing(color, 0, part)[...]
                picks = [slice(None)] * (dims - 1)
                result[(color, *picks, strip_rows[part])] = total + landing(color, 1, part)[...]

        return far, close, pass_on, finish

    def nothing(color, j, part):
        pass

    def direct(color, step, part):
        at = (me[axes[color][2]] + step) % 4
        src = sum2.at[color, at, strip_rows[part]]
        return hop(2, color, step - 1, step, part, src, final3.at[color, step - 1, strip_rows[part]])

    def last_out(part):
        for step in (2, 1, 3):
            for color in range(COLORS):
                direct(color, step, part).start()
                waiting.append(direct(color, step, part))

    def last_in(part):
        for color in range(COLORS):
            total = sum2[color, me[axes[color][2]], strip_rows[part]]
            for step in (1, 3, 2):
                direct(color, step, part).wait_recv()
                total = total + final3[color, step - 1, strip_rows[part]]
            sum3[color, strip_rows[part]] = total

    far1, close1, pass1, finish1 = ring(0, own, relay1, final1, sum1, arrived)
    far2, close2, pass2, finish2 = ring(1, sum1, relay2, final2, sum2, nothing)
    far1(0), close1(0), far1(1), pass1(0), close1(1), finish1(0)
    far2(0), close2(0), pass1(1), pass2(0), finish1(1)
    far2(1), close2(1), finish2(0), last_out(0), pass2(1), last_in(0)
    finish2(1), last_out(1), last_in(1)

    low_half = r < 8
    group = jnp.where(low_half, r, 15 - r)
    strip = jnp.where(low_half, c, c + 8)

    def piece(t):
        return sum3.at[t // PIECES, pl.ds((t % PIECES) * 8, 8)]

    def tile_copy(t, mirrored):
        first = t < 16 - group
        i = jnp.where(first, group, 15 - group)
        j = jnp.where(first, group + t, t - 1)
        row, column = (j, i) if mirrored else (i, j)
        copy = pltpu.make_async_remote_copy(
            src_ref=piece(t),
            dst_ref=land.at[column % 2, strip],
            send_sem=tile_send.at[t, int(mirrored)],
            recv_sem=tile_recv.at[column % 2, strip],
            device_id={"row": row, "col": column // 2},
            device_id_type=MESH,
        )
        mine = (row == r) & (column // 2 == c)
        wanted = (i != j) if mirrored else None
        return copy, mine, wanted, column % 2

    holder = c == r // 2

    def to_column(d):
        return pltpu.make_async_remote_copy(
            src_ref=block_out,
            dst_ref=blocks_in.at[1 + r % 2],
            send_sem=block_send.at[d],
            recv_sem=block_recv.at[1 + r % 2],
            device_id={"row": (r + d) % 16, "col": c},
            device_id_type=MESH,
        )

    def to_row(d):
        return pltpu.make_async_remote_copy(
            src_ref=block_out,
            dst_ref=blocks_in.at[0],
            send_sem=block_send.at[15 + d],
            recv_sem=block_recv.at[0],
            device_id={"row": r, "col": (c + d) % 8},
            device_id_type=MESH,
        )

    @pl.when(holder)
    def hand_out():
        reduced = rhs[...] - sum3[2, 40:41, :]
        row = lax.broadcasted_iota(jnp.int32, (8, BLOCK), 0)
        value = jnp.where(row == 0, reduced, jnp.where(row == 1, prior[...], weight[...]))
        block_out[...] = value
        blocks_in[0] = value
        blocks_in[1 + r % 2] = value
        for d in range(1, 16):
            to_column(d).start()
        for d in range(1, 8):
            to_row(d).start()

    for t in range(17):
        for mirrored in (False, True):
            copy, mine, wanted, side = tile_copy(t, mirrored)
            away = jnp.logical_not(mine)
            if wanted is not None:
                mine, away = mine & wanted, away & wanted

            @pl.when(away)
            def send():
                copy.start()

            @pl.when(mine)
            def keep():
                land[side, strip] = piece(t)[...]

    def receive(buffer, semaphore):
        pltpu.make_async_remote_copy(
            src_ref=buffer,
            dst_ref=buffer,
            send_sem=semaphore,
            recv_sem=semaphore,
            device_id=partner,
            device_id_type=MESH,
        ).wait_recv()

    for side in range(2):
        column = 2 * c + side
        low = jnp.minimum(r, column)
        owner = jnp.where(low < 8, low, 15 - low)
        for s in range(16):
            row = owner if s < 8 else 15 - owner

            @pl.when(jnp.logical_not((row == r) & (c == s % 8)))
            def wait():
                receive(land.at[side, s], tile_recv.at[side, s])

    tiles = []
    for side in range(2):
        found = land[side].reshape(BLOCK, BLOCK)
        found = jnp.where(r > 2 * c + side, found.T, found)
        lanes = slice(side * BLOCK, (side + 1) * BLOCK)
        tile = matrix[:, lanes] - found
        out_matrix[:, lanes] = tile
        tiles.append(tile)

    @pl.when(jnp.logical_not(holder))
    def row_block():
        receive(blocks_in.at[0], block_recv.at[0])

    for side in range(2):

        @pl.when(r != 2 * c + side)
        def column_block():
            receive(blocks_in.at[1 + side], block_recv.at[1 + side])

    reduced = blocks_in[0, 0:1, :]
    out_rhs[...] = reduced

    def matvec(first, second):
        spread = tiles[0] * first + tiles[1] * second
        return jnp.broadcast_to(jnp.sum(spread.T, axis=0, keepdims=True), (8, BLOCK))

    def along_row(d, source, target, sends, recvs):
        return pltpu.make_async_remote_copy(
            src_ref=source,
            dst_ref=target.at[c],
            send_sem=sends.at[d],
            recv_sem=recvs.at[c],
            device_id={"row": r, "col": (c + d) % 8},
            device_id_type=MESH,
        )

    def along_column(d):
        return pltpu.make_async_remote_copy(
            src_ref=partial1,
            dst_ref=column1.at[r % 2, c],
            send_sem=column_send.at[d],
            recv_sem=column_recv.at[r % 2, c],
            device_id={"row": (r + d) % 16, "col": r // 2},
            device_id_type=MESH,
        )

    value = matvec(blocks_in[1, 1:2, :], blocks_in[2, 1:2, :])
    partial1[...] = value
    row1[c] = value
    for d in range(1, 16):
        along_column(d).start()

    @pl.when(jnp.logical_not(holder))
    def last_column():
        along_column(0).start()

    @pl.when(holder)
    def own_column():
        column1[r % 2, c] = value

    for d in range(1, 8):
        along_row(d, partial1, row1, one_send, one_recv).start()

    def gather_row(target, recvs):
        for s in range(8):

            @pl.when(c != s)
            def wait():
                receive(target.at[s], recvs.at[s])

    def total(ref):
        value = ref[0, 0:1, :]
        for s in range(1, 8):
            value = value + ref[s, 0:1, :]
        return value

    def updated(block, product):
        return block[1:2, :] + block[2:3, :] * (block[0:1, :] - product)

    for side in range(2):
        for s in range(8):

            @pl.when(jnp.logical_not((r == 2 * c + side) & (c == s)))
            def wait():
                receive(column1.at[side, s], column_recv.at[side, s])

    first = [updated(blocks_in[1 + side], total(column1.at[side])) for side in range(2)]
    value = matvec(*first)
    partial2[...] = value
    row2[c] = value
    for d in range(1, 8):
        along_row(d, partial2, row2, two_send, two_recv).start()
    gather_row(row1, one_recv)
    mine = updated(blocks_in[0], total(row1))
    gather_row(row2, two_recv)
    out_solution[...] = mine + weight[...] * (reduced - total(row2))

    for j, part in everything:
        for color in range(COLORS):
            pairs(color, j, part).wait_send()
    for copy in waiting:
        copy.wait_send()
    for t in range(17):
        for mirrored in (False, True):
            copy, mine, wanted, side = tile_copy(t, mirrored)
            away = jnp.logical_not(mine)
            if wanted is not None:
                away = away & wanted

            @pl.when(away)
            def sent():
                copy.wait_send()

    @pl.when(holder)
    def handed():
        for d in range(1, 16):
            to_column(d).wait_send()
        for d in range(1, 8):
            to_row(d).wait_send()

    for d in range(1, 16):
        along_column(d).wait_send()

    @pl.when(jnp.logical_not(holder))
    def last_sent():
        along_column(0).wait_send()

    for d in range(1, 8):
        along_row(d, partial1, row1, one_send, one_recv).wait_send()
        along_row(d, partial2, row2, two_send, two_recv).wait_send()


def partial_sum(local_inverse, coupling, local_rhs, members):
    def two(rows, columns, dtype=bf16):
        return (pltpu.VMEM((rows, columns), dtype),) * 2

    columns = TOUCHED * BLOCK
    return pl.pallas_call(
        eliminate,
        in_specs=[
            pl.BlockSpec(memory_space=pltpu.SMEM),
            pl.BlockSpec(memory_space=pltpu.HBM),
            pl.BlockSpec(memory_space=pltpu.HBM),
            pl.BlockSpec(memory_space=pltpu.VMEM),
        ],
        out_specs=pl.BlockSpec(memory_space=pltpu.VMEM),
        scratch_shapes=[
            two(LOCAL, LOCAL, f32),
            two(LOCAL, columns, f32),
            pltpu.SemaphoreType.DMA((2, 2)),
            (two(HEAD + columns, LOCAL),) * 2,
            (two(LOCAL, columns),) * 2,
            (two(LOCAL, LOCAL),) * 2,
            two(HEAD + columns, LOCAL),
        ],
        out_shape=jax.ShapeDtypeStruct((GRID, 8, BLOCK), f32),
        compiler_params=pltpu.CompilerParams(vmem_limit_bytes=34 * 2**20),
        name="eliminate",
    )(members, local_inverse, coupling, local_rhs)


def combined(summed, shared_matrix, shared_rhs, prior_solution, preconditioner):
    rows, columns = shared_matrix.shape
    vmem = pl.BlockSpec(memory_space=pltpu.VMEM)
    strip = PIECES * 8
    dma = pltpu.SemaphoreType.DMA

    def buffer(*shape):
        return pltpu.VMEM(shape, f32)

    return pl.pallas_call(
        combine,
        in_specs=[pl.BlockSpec(memory_space=pl.ANY)] + [vmem] * 4,
        out_specs=[vmem] * 3,
        out_shape=[
            jax.ShapeDtypeStruct((rows, columns), f32),
            jax.ShapeDtypeStruct((1, rows), f32),
            jax.ShapeDtypeStruct((1, rows), f32),
        ],
        scratch_shapes=[
            buffer(COLORS, 4, 4, 4, strip, BLOCK),
            buffer(COLORS, 4, 4, 4, strip, BLOCK),
            buffer(COLORS, 2, 2, 4, strip, BLOCK),
            buffer(COLORS, 2, 4, 4, strip, BLOCK),
            buffer(COLORS, 4, 4, strip, BLOCK),
            buffer(COLORS, 2, 2, strip, BLOCK),
            buffer(COLORS, 2, 4, strip, BLOCK),
            buffer(COLORS, 4, strip, BLOCK),
            buffer(COLORS, 3, strip, BLOCK),
            buffer(COLORS, strip, BLOCK),
            buffer(2, 16, 8, BLOCK),
            buffer(8, BLOCK),
            buffer(3, 8, BLOCK),
            buffer(8, BLOCK),
            buffer(8, BLOCK),
            buffer(8, 8, BLOCK),
            buffer(2, 8, 8, BLOCK),
            buffer(8, 8, BLOCK),
            dma((2, COLORS, 4)),
            dma((2, COLORS, 4)),
            dma((2, COLORS, 4)),
            dma((2, 3, COLORS, 6)),
            dma((2, 3, COLORS, 6)),
            dma((17, 2)),
            dma((2, 16)),
            dma((23,)),
            dma((3,)),
            dma((8,)),
            dma((8,)),
            dma((16,)),
            dma((2, 8)),
            dma((8,)),
            dma((8,)),
        ],
        compiler_params=pltpu.CompilerParams(
            collective_id=0, has_side_effects=True, vmem_limit_bytes=24 * 2**20
        ),
        name="combine",
    )(
        summed.reshape(COLORS, 2, 4, 4, 4, strip, BLOCK),
        shared_matrix,
        shared_rhs.reshape(1, rows),
        prior_solution.reshape(1, rows),
        preconditioner.reshape(1, rows),
    )


def local(
    local_inverse,
    coupling,
    local_rhs,
    members,
    shared_matrix,
    shared_rhs,
    prior_solution,
    preconditioner,
):
    summed = partial_sum(local_inverse, coupling, local_rhs, members)
    reduced_matrix, reduced_rhs, solution = combined(
        summed, shared_matrix, shared_rhs, prior_solution, preconditioner
    )
    return reduced_matrix, reduced_rhs.reshape(-1), solution.reshape(-1)


def solution(mesh):
    both = ("row", "col")
    placed = (
        P(both, None, None),
        P(both, None, None),
        P(both, None),
        P(both, None),
        P("row", "col"),
        P("row"),
        P("row"),
        P("row"),
    )
    return jax.shard_map(
        local,
        mesh=mesh,
        in_specs=placed,
        out_specs=(P("row", "col"), P("row"), P("row")),
        check_vma=False,
    )
```

```python
import functools

import jax
import jax.numpy as jnp
from jax import lax
from jax.experimental import pallas as pl
from jax.experimental.pallas import tpu as pltpu
from jax.sharding import PartitionSpec as P

BLOCK = 128
BLOCKS = 16
TOUCHED = 8
LOCAL = 512
PASSES = 3
HEAD = 16
COLORS = 3
PIECES = 6
GRID = COLORS * 2 * 64 * PIECES
MESH = pl.DeviceIdType.MESH
f32 = jnp.float32
bf16 = jnp.bfloat16


def split(value):
    high = value.astype(bf16)
    return high, (value - high.astype(f32)).astype(bf16)


def product(left, right):
    total = jnp.dot(left[0], right[0], preferred_element_type=f32)
    if PASSES == 3:
        total += jnp.dot(left[1], right[0], preferred_element_type=f32)
        total += jnp.dot(left[0], right[1], preferred_element_type=f32)
    return total


def piece_base(block):
    core, z = block % 2, (block // 2) % 4
    return core * 384 + (block // 8) * 192 + z * PIECES


def eliminate(
    members, inverse, coupling, rhs, summed,
    inverse_in, coupling_in, in_sem,
    turned, held, kept, mapped,
):
    weeks = inverse.shape[0]

    def fetch(week):
        return (
            pltpu.make_async_copy(inverse.at[week], inverse_in.at[week], in_sem.at[week, 0]),
            pltpu.make_async_copy(coupling.at[week], coupling_in.at[week], in_sem.at[week, 1]),
        )

    def order(week):
        blocks = [members[week, k] for k in range(TOUCHED)]
        ranks = [
            sum((blocks[j] < blocks[k]).astype(jnp.int32) for j in range(TOUCHED) if j != k)
            for k in range(TOUCHED)
        ]
        place, sorted_blocks = [], []
        for a in range(TOUCHED):
            here = [(ranks[k] == a).astype(jnp.int32) for k in range(TOUCHED)]
            place.append(sum(here[k] * k for k in range(1, TOUCHED)))
            sorted_blocks.append(sum(here[k] * blocks[k] for k in range(TOUCHED)))
        return place, sorted_blocks

    def prepare(week, slot):
        place, _ = order(week)

        def columns_of(a):
            def work():
                columns = coupling_in[week, :, pl.ds(pl.multiple_of(place[a] * BLOCK, BLOCK), BLOCK)]
                at = slice(a * BLOCK, (a + 1) * BLOCK)
                held[slot][0][:, at], held[slot][1][:, at] = split(columns)
                at = slice(HEAD + a * BLOCK, HEAD + (a + 1) * BLOCK)
                turned[slot][0][at, :], turned[slot][1][at, :] = split(columns.T)

            return work

        def inverse_part(n):
            def work():
                at = slice(n * 128, n * 128 + 128)
                kept[slot][0][at, :], kept[slot][1][at, :] = split(inverse_in[week, at, :])

            return work

        def head():
            row = lax.broadcasted_iota(jnp.int32, (HEAD, LOCAL), 0)
            first = jnp.where(row == 0, jnp.broadcast_to(rhs[pl.ds(week, 1), :], (HEAD, LOCAL)), 0.0)
            turned[slot][0][0:HEAD, :], turned[slot][1][0:HEAD, :] = split(first)

        return [head] + [inverse_part(n) for n in range(4)] + [columns_of(a) for a in range(TOUCHED)]

    def multiply(week, slot):
        _, blocks = order(week)

        def map_part(n, rows):
            def work():
                at = slice(n * 256, n * 256 + 256)
                part = product(
                    (turned[slot][0][rows, :], turned[slot][1][rows, :]),
                    (kept[slot][0][:, at], kept[slot][1][:, at]),
                )
                mapped[0][rows, at], mapped[1][rows, at] = split(part)

            return work

        def add_tiles(n, part, offset, places):
            for b in (2 * n, 2 * n + 1):
                lanes = slice((b - 2 * n) * BLOCK, (b - 2 * n + 1) * BLOCK)
                for a in places:
                    if a == -1:
                        index = 2 * 768 + piece_base(blocks[b]) + (blocks[b] // 8) * 96
                        index += ((blocks[b] // 2) % 4) * 24 + PIECES - 1
                        summed[index] = summed[index] + part[0:8, lanes]
                    elif a <= b:
                        low_half = blocks[a] < 8
                        group = jnp.where(low_half, blocks[a], 15 - blocks[a])
                        piece = jnp.where(low_half, blocks[b] - blocks[a], blocks[b] + 1)
                        first = (piece // PIECES) * 768 + piece % PIECES
                        top = HEAD + a * BLOCK - offset
                        tile = part[top : top + BLOCK, lanes].reshape(16, 8, BLOCK)
                        spots = []
                        for s in range(16):
                            base = first + piece_base(group if s < 8 else 15 - group)
                            spots.append(base + (s % 8 // 4) * 96 + (s % 4) * 24)
                        new = [summed[spots[s]] + tile[s] for s in range(16)]
                        for s in range(16):
                            summed[spots[s]] = new[s]

        def pair_part(n, m):
            def work():
                low = 0 if m == 0 else HEAD + m * 256
                rows = slice(low, HEAD + (m + 1) * 256)
                at = slice(n * 256, n * 256 + 256)
                part = product(
                    (mapped[0][rows, :], mapped[1][rows, :]),
                    (held[slot][0][:, at], held[slot][1][:, at]),
                )
                add_tiles(n, part, low, ([-1] if m == 0 else []) + [2 * m, 2 * m + 1])

            return work

        cuts = [slice(0, HEAD + 256)] + [slice(HEAD + k * 256, HEAD + k * 256 + 256) for k in (1, 2, 3)]
        first = [map_part(n, rows) for rows in cuts for n in range(2)]
        return first + [pair_part(n, m) for n in range(4) for m in range(n + 1)]

    def half_step(week, slot):
        other = 1 - slot

        @pl.when(week + 1 < weeks)
        def arrive():
            for copy in fetch(week + 1):
                copy.wait()

        work = multiply(week, slot)
        more = prepare(jnp.minimum(week + 1, weeks - 1), other)
        for index, item in enumerate(work):
            item()
            if index < len(more):
                more[index]()

    for week in range(2):
        for copy in fetch(week):
            copy.start()

    @pl.loop(0, GRID // 16)
    def clear(index):
        summed[pl.ds(index * 16, 16)] = jnp.zeros((16, 8, BLOCK), f32)

    for copy in fetch(0):
        copy.wait()
    for week in range(2, weeks):
        for copy in fetch(week):
            copy.start()
    for item in prepare(0, 0):
        item()

    @pl.loop(0, weeks // 2)
    def step(index):
        half_step(2 * index, 0)
        half_step(2 * index + 1, 1)


def device(x, y, z, core):
    return {"row": (x // 2) * 8 + z * 2 + core, "col": (x % 2) * 4 + y}


def combine(
    data, matrix, rhs, prior, weight,
    out_matrix, out_rhs, out_solution,
    own, other, relay1, final1, sum1, relay2, final2, sum2, final3, sum3,
    land, block_out, blocks_in, partial1, partial2, row1, column1, row2,
    pair_send, pair_recv, ring_send, ring_recv,
    tile_send, tile_recv, block_send, block_recv,
    one_send, one_recv, column_send, column_recv, two_send, two_recv,
):
    r, c = lax.axis_index("row"), lax.axis_index("col")
    core, z = r % 2, (r // 2) % 4
    x, y = (r // 8) * 2 + c // 4, c % 4
    me = (x, y, z)

    def neighbour(axis, step):
        at = list(me)
        at[axis] = (me[axis] + step) % 4
        return device(*at, core)

    barrier = pltpu.get_barrier_semaphore()
    partner = {"row": r + 1 - 2 * core, "col": c}
    greeted = [partner] + [neighbour(axis, step) for axis in range(3) for step in (1, 3)]
    for target in greeted:
        pl.semaphore_signal(barrier, inc=1, device_id=target, device_id_type=MESH)

    strip_rows = [pl.ds(24 * part, 24) for part in range(2)]

    def cut(ref, lead, dims, position, index, part, half=None):
        picks = [slice(None)] * dims
        picks[position] = index
        if half is not None:
            picks[0 if position else 1] = pl.ds(2 * half, 2)
        return ref.at[(*lead, *picks, strip_rows[part])]

    def pairs(color, j, part):
        at = (me[color] + j) % 4
        return pltpu.make_async_remote_copy(
            src_ref=cut(data, (color, 1 - core), 3, color, at, part),
            dst_ref=cut(other, (color,), 3, color, at, part),
            send_sem=pair_send.at[part, color, j],
            recv_sem=pair_recv.at[part, color, j],
            device_id=partner,
            device_id_type=MESH,
        )

    everything = [(2, 0), (1, 0), (3, 0), (2, 1), (0, 0), (1, 1), (3, 1), (0, 1)]
    pl.semaphore_wait(barrier, len(greeted))
    for j, part in everything:
        for color in range(COLORS):
            pairs(color, j, part).start()

    def add(target, *terms):
        value = target[...]
        for term in terms:
            value = value + term[...]
        target[...] = value

    def arrived(color, j, part):
        at = (me[color] + j) % 4
        pairs(color, j, part).wait_recv()
        mine = cut(data, (color, core), 3, color, at, part)
        total = mine[...] + cut(other, (color,), 3, color, at, part)[...]
        cut(own, (color,), 3, color, at, part)[...] = total

    axes = ((0, 1, 2), (1, 2, 0), (2, 0, 1))
    spots = ((0, 0), (1, 1), (2, 0))
    waiting = []

    def hop(number, color, slot, step, part, src, dst):
        return pltpu.make_async_remote_copy(
            src_ref=src,
            dst_ref=dst,
            send_sem=ring_send.at[part, number, color, slot],
            recv_sem=ring_recv.at[part, number, color, slot],
            device_id=neighbour(axes[color][number], step),
            device_id_type=MESH,
        )

    def ring(number, source, relay, final, result, prepare):
        dims = 3 - number

        def source_cut(color, step, part, half=None):
            at = (me[axes[color][number]] + step) % 4
            return cut(source, (color,), dims, spots[color][number], at, part, half)

        def landing(color, side, part, half=None):
            picks = [slice(None)] * (dims - 1)
            if half is not None:
                picks[0] = pl.ds(2 * half, 2)
            return final.at[(color, side, *picks, strip_rows[part])]

        def relayed(color, side, part):
            return relay.at[(color, side, *[slice(None)] * (dims - 1), strip_rows[part])]

        def away(color, side, part):
            src = source_cut(color, 2, part, side)
            return hop(number, color, side, (1, 3)[side], part, src, relayed(color, side, part))

        def near(color, side, part, half):
            step = (1, 3)[side]
            src = source_cut(color, step, part, half)
            dst = landing(color, side, part, half)
            return hop(number, color, 2 + 2 * side + half, step, part, src, dst)

        def far(part):
            for color in range(COLORS):
                prepare(color, 2, part)
                for side in range(2):
                    away(color, side, part).start()
                    waiting.append(away(color, side, part))

        def close(part):
            for color in range(COLORS):
                for side in range(2):
                    prepare(color, (1, 3)[side], part)
                    near(color, side, part, 1 - side).start()

        def pass_on(part):
            for color in range(COLORS):
                for side in range(2):
                    away(color, side, part).wait_recv()
                    add(source_cut(color, (1, 3)[side], part, side), relayed(color, side, part))
                    near(color, side, part, side).start()

        def finish(part):
            for color in range(COLORS):
                prepare(color, 0, part)
                for side in range(2):
                    for half in range(2):
                        near(color, side, part, half).wait_recv()
                        waiting.append(near(color, side, part, half))
                total = source_cut(color, 0, part)[...] + landing(color, 0, part)[...]
                picks = [slice(None)] * (dims - 1)
                result[(color, *picks, strip_rows[part])] = total + landing(color, 1, part)[...]

        return far, close, pass_on, finish

    def nothing(color, j, part):
        pass

    def direct(color, step, part):
        at = (me[axes[color][2]] + step) % 4
        src = sum2.at[color, at, strip_rows[part]]
        return hop(2, color, step - 1, step, part, src, final3.at[color, step - 1, strip_rows[part]])

    def last_out(part):
        for step in (2, 1, 3):
            for color in range(COLORS):
                direct(color, step, part).start()
                waiting.append(direct(color, step, part))

    def last_in(part):
        for color in range(COLORS):
            total = sum2[color, me[axes[color][2]], strip_rows[part]]
            for step in (1, 3, 2):
                direct(color, step, part).wait_recv()
                total = total + final3[color, step - 1, strip_rows[part]]
            sum3[color, strip_rows[part]] = total

    far1, close1, pass1, finish1 = ring(0, own, relay1, final1, sum1, arrived)
    far2, close2, pass2, finish2 = ring(1, sum1, relay2, final2, sum2, nothing)
    far1(0), close1(0), far1(1), pass1(0), close1(1), finish1(0)
    far2(0), close2(0), pass1(1), pass2(0), finish1(1)
    far2(1), close2(1), finish2(0), last_out(0), pass2(1), last_in(0)
    finish2(1), last_out(1), last_in(1)

    low_half = r < 8
    group = jnp.where(low_half, r, 15 - r)
    strip = jnp.where(low_half, c, c + 8)

    def piece(t):
        return sum3.at[t // PIECES, pl.ds((t % PIECES) * 8, 8)]

    def tile_copy(t, mirrored):
        first = t < 16 - group
        i = jnp.where(first, group, 15 - group)
        j = jnp.where(first, group + t, t - 1)
        row, column = (j, i) if mirrored else (i, j)
        copy = pltpu.make_async_remote_copy(
            src_ref=piece(t),
            dst_ref=land.at[column % 2, strip],
            send_sem=tile_send.at[t, int(mirrored)],
            recv_sem=tile_recv.at[column % 2, strip],
            device_id={"row": row, "col": column // 2},
            device_id_type=MESH,
        )
        mine = (row == r) & (column // 2 == c)
        wanted = (i != j) if mirrored else None
        return copy, mine, wanted, column % 2

    holder = c == r // 2

    def to_column(d):
        return pltpu.make_async_remote_copy(
            src_ref=block_out,
            dst_ref=blocks_in.at[1 + r % 2],
            send_sem=block_send.at[d],
            recv_sem=block_recv.at[1 + r % 2],
            device_id={"row": (r + d) % 16, "col": c},
            device_id_type=MESH,
        )

    def to_row(d):
        return pltpu.make_async_remote_copy(
            src_ref=block_out,
            dst_ref=blocks_in.at[0],
            send_sem=block_send.at[15 + d],
            recv_sem=block_recv.at[0],
            device_id={"row": r, "col": (c + d) % 8},
            device_id_type=MESH,
        )

    @pl.when(holder)
    def hand_out():
        reduced = rhs[...] - sum3[2, 40:41, :]
        row = lax.broadcasted_iota(jnp.int32, (8, BLOCK), 0)
        value = jnp.where(row == 0, reduced, jnp.where(row == 1, prior[...], weight[...]))
        block_out[...] = value
        blocks_in[0] = value
        blocks_in[1 + r % 2] = value
        for d in range(1, 16):
            to_column(d).start()
        for d in range(1, 8):
            to_row(d).start()

    for t in range(17):
        for mirrored in (False, True):
            copy, mine, wanted, side = tile_copy(t, mirrored)
            away = jnp.logical_not(mine)
            if wanted is not None:
                mine, away = mine & wanted, away & wanted

            @pl.when(away)
            def send():
                copy.start()

            @pl.when(mine)
            def keep():
                land[side, strip] = piece(t)[...]

    def receive(buffer, semaphore):
        pltpu.make_async_remote_copy(
            src_ref=buffer,
            dst_ref=buffer,
            send_sem=semaphore,
            recv_sem=semaphore,
            device_id=partner,
            device_id_type=MESH,
        ).wait_recv()

    for side in range(2):
        column = 2 * c + side
        low = jnp.minimum(r, column)
        owner = jnp.where(low < 8, low, 15 - low)
        for s in range(16):
            row = owner if s < 8 else 15 - owner

            @pl.when(jnp.logical_not((row == r) & (c == s % 8)))
            def wait():
                receive(land.at[side, s], tile_recv.at[side, s])

    tiles = []
    for side in range(2):
        found = land[side].reshape(BLOCK, BLOCK)
        found = jnp.where(r > 2 * c + side, found.T, found)
        lanes = slice(side * BLOCK, (side + 1) * BLOCK)
        tile = matrix[:, lanes] - found
        out_matrix[:, lanes] = tile
        tiles.append(tile)

    @pl.when(jnp.logical_not(holder))
    def row_block():
        receive(blocks_in.at[0], block_recv.at[0])

    for side in range(2):

        @pl.when(r != 2 * c + side)
        def column_block():
            receive(blocks_in.at[1 + side], block_recv.at[1 + side])

    reduced = blocks_in[0, 0:1, :]
    out_rhs[...] = reduced

    def matvec(first, second):
        spread = tiles[0] * first + tiles[1] * second
        return jnp.broadcast_to(jnp.sum(spread.T, axis=0, keepdims=True), (8, BLOCK))

    def along_row(d, source, target, sends, recvs):
        return pltpu.make_async_remote_copy(
            src_ref=source,
            dst_ref=target.at[c],
            send_sem=sends.at[d],
            recv_sem=recvs.at[c],
            device_id={"row": r, "col": (c + d) % 8},
            device_id_type=MESH,
        )

    def along_column(d):
        return pltpu.make_async_remote_copy(
            src_ref=partial1,
            dst_ref=column1.at[r % 2, c],
            send_sem=column_send.at[d],
            recv_sem=column_recv.at[r % 2, c],
            device_id={"row": (r + d) % 16, "col": r // 2},
            device_id_type=MESH,
        )

    value = matvec(blocks_in[1, 1:2, :], blocks_in[2, 1:2, :])
    partial1[...] = value
    row1[c] = value
    for d in range(1, 16):
        along_column(d).start()

    @pl.when(jnp.logical_not(holder))
    def last_column():
        along_column(0).start()

    @pl.when(holder)
    def own_column():
        column1[r % 2, c] = value

    for d in range(1, 8):
        along_row(d, partial1, row1, one_send, one_recv).start()

    def gather_row(target, recvs):
        for s in range(8):

            @pl.when(c != s)
            def wait():
                receive(target.at[s], recvs.at[s])

    def total(ref):
        value = ref[0, 0:1, :]
        for s in range(1, 8):
            value = value + ref[s, 0:1, :]
        return value

    def updated(block, product):
        return block[1:2, :] + block[2:3, :] * (block[0:1, :] - product)

    for side in range(2):
        for s in range(8):

            @pl.when(jnp.logical_not((r == 2 * c + side) & (c == s)))
            def wait():
                receive(column1.at[side, s], column_recv.at[side, s])

    first = [updated(blocks_in[1 + side], total(column1.at[side])) for side in range(2)]
    value = matvec(*first)
    partial2[...] = value
    row2[c] = value
    for d in range(1, 8):
        along_row(d, partial2, row2, two_send, two_recv).start()
    gather_row(row1, one_recv)
    mine = updated(blocks_in[0], total(row1))
    gather_row(row2, two_recv)
    out_solution[...] = mine + weight[...] * (reduced - total(row2))

    for j, part in everything:
        for color in range(COLORS):
            pairs(color, j, part).wait_send()
    for copy in waiting:
        copy.wait_send()
    for t in range(17):
        for mirrored in (False, True):
            copy, mine, wanted, side = tile_copy(t, mirrored)
            away = jnp.logical_not(mine)
            if wanted is not None:
                away = away & wanted

            @pl.when(away)
            def sent():
                copy.wait_send()

    @pl.when(holder)
    def handed():
        for d in range(1, 16):
            to_column(d).wait_send()
        for d in range(1, 8):
            to_row(d).wait_send()

    for d in range(1, 16):
        along_column(d).wait_send()

    @pl.when(jnp.logical_not(holder))
    def last_sent():
        along_column(0).wait_send()

    for d in range(1, 8):
        along_row(d, partial1, row1, one_send, one_recv).wait_send()
        along_row(d, partial2, row2, two_send, two_recv).wait_send()


def partial_sum(local_inverse, coupling, local_rhs, members):
    local_inverse = pltpu.with_memory_space_constraint(local_inverse, pltpu.HBM)
    coupling = pltpu.with_memory_space_constraint(coupling, pltpu.HBM)
    members = pltpu.with_memory_space_constraint(members, pltpu.HBM)
    local_rhs = pltpu.with_memory_space_constraint(local_rhs, pltpu.HBM)

    def two(rows, columns, dtype=bf16):
        return (pltpu.VMEM((rows, columns), dtype),) * 2

    weeks, columns = local_inverse.shape[0], TOUCHED * BLOCK
    return pl.pallas_call(
        eliminate,
        grid_spec=pltpu.PrefetchScalarGridSpec(
            num_scalar_prefetch=1,
            grid=(1,),
            in_specs=[
                pl.BlockSpec(memory_space=pl.ANY),
                pl.BlockSpec(memory_space=pl.ANY),
                pl.BlockSpec(local_rhs.shape, lambda step, m: (0, 0)),
            ],
            out_specs=pl.BlockSpec(memory_space=pltpu.VMEM),
            scratch_shapes=[
                pltpu.VMEM((weeks, LOCAL, LOCAL), f32),
                pltpu.VMEM((weeks, LOCAL, columns), f32),
                pltpu.SemaphoreType.DMA((weeks, 2)),
                (two(HEAD + columns, LOCAL),) * 2,
                (two(LOCAL, columns),) * 2,
                (two(LOCAL, LOCAL),) * 2,
                two(HEAD + columns, LOCAL),
            ],
        ),
        out_shape=jax.ShapeDtypeStruct((GRID, 8, BLOCK), f32),
        compiler_params=pltpu.CompilerParams(
            vmem_limit_bytes=42 * 2**20
        ),
        name="eliminate",
    )(members, local_inverse, coupling, local_rhs)


def combined(summed, shared_matrix, shared_rhs, prior_solution, preconditioner):
    rows, columns = shared_matrix.shape
    vmem = pl.BlockSpec(memory_space=pltpu.VMEM)
    strip = PIECES * 8
    dma = pltpu.SemaphoreType.DMA

    def buffer(*shape):
        return pltpu.VMEM(shape, f32)

    return pl.pallas_call(
        combine,
        in_specs=[vmem] * 5,
        out_specs=[vmem] * 3,
        out_shape=[
            jax.ShapeDtypeStruct((rows, columns), f32),
            jax.ShapeDtypeStruct((1, rows), f32),
            jax.ShapeDtypeStruct((1, rows), f32),
        ],
        scratch_shapes=[
            buffer(COLORS, 4, 4, 4, strip, BLOCK),
            buffer(COLORS, 4, 4, 4, strip, BLOCK),
            buffer(COLORS, 2, 2, 4, strip, BLOCK),
            buffer(COLORS, 2, 4, 4, strip, BLOCK),
            buffer(COLORS, 4, 4, strip, BLOCK),
            buffer(COLORS, 2, 2, strip, BLOCK),
            buffer(COLORS, 2, 4, strip, BLOCK),
            buffer(COLORS, 4, strip, BLOCK),
            buffer(COLORS, 3, strip, BLOCK),
            buffer(COLORS, strip, BLOCK),
            buffer(2, 16, 8, BLOCK),
            buffer(8, BLOCK),
            buffer(3, 8, BLOCK),
            buffer(8, BLOCK),
            buffer(8, BLOCK),
            buffer(8, 8, BLOCK),
            buffer(2, 8, 8, BLOCK),
            buffer(8, 8, BLOCK),
            dma((2, COLORS, 4)),
            dma((2, COLORS, 4)),
            dma((2, 3, COLORS, 6)),
            dma((2, 3, COLORS, 6)),
            dma((17, 2)),
            dma((2, 16)),
            dma((23,)),
            dma((3,)),
            dma((8,)),
            dma((8,)),
            dma((16,)),
            dma((2, 8)),
            dma((8,)),
            dma((8,)),
        ],
        compiler_params=pltpu.CompilerParams(
            collective_id=0, has_side_effects=True, vmem_limit_bytes=24 * 2**20
        ),
        name="combine",
    )(
        summed.reshape(COLORS, 2, 4, 4, 4, strip, BLOCK),
        shared_matrix,
        shared_rhs.reshape(1, rows),
        prior_solution.reshape(1, rows),
        preconditioner.reshape(1, rows),
    )


def local(
    local_inverse,
    coupling,
    local_rhs,
    members,
    shared_matrix,
    shared_rhs,
    prior_solution,
    preconditioner,
):
    summed = partial_sum(local_inverse, coupling, local_rhs, members)
    reduced_matrix, reduced_rhs, solution = combined(
        summed, shared_matrix, shared_rhs, prior_solution, preconditioner
    )
    return reduced_matrix, reduced_rhs.reshape(-1), solution.reshape(-1)


def solution(mesh):
    both = ("row", "col")
    placed = (
        P(both, None, None),
        P(both, None, None),
        P(both, None),
        P(both, None),
        P("row", "col"),
        P("row"),
        P("row"),
        P("row"),
    )
    return jax.shard_map(
        local,
        mesh=mesh,
        in_specs=placed,
        out_specs=(P("row", "col"), P("row"), P("row")),
        check_vma=False,
    )
```

```python
import functools

import jax
import jax.numpy as jnp
from jax import lax
from jax.experimental import pallas as pl
from jax.experimental.pallas import tpu as pltpu
from jax.sharding import PartitionSpec as P

BLOCK = 128
BLOCKS = 16
TOUCHED = 8
LOCAL = 512
PASSES = 3
HEAD = 16
COLORS = 3
PIECES = 6
GRID = COLORS * 2 * 64 * PIECES
MESH = pl.DeviceIdType.MESH
f32 = jnp.float32
bf16 = jnp.bfloat16


def split(value):
    high = value.astype(bf16)
    return high, (value - high.astype(f32)).astype(bf16)


def product(left, right):
    total = jnp.dot(left[0], right[0], preferred_element_type=f32)
    if PASSES == 3:
        total += jnp.dot(left[1], right[0], preferred_element_type=f32)
        total += jnp.dot(left[0], right[1], preferred_element_type=f32)
    return total


def piece_base(block):
    core, z = block % 2, (block // 2) % 4
    return core * 384 + (block // 8) * 192 + z * PIECES


def eliminate(
    members, inverse, coupling, rhs, summed,
    inverse_in, coupling_in, in_sem,
    turned, held, kept, mapped,
):
    weeks = inverse.shape[0]

    def fetch(week):
        return (
            pltpu.make_async_copy(inverse.at[week], inverse_in.at[week], in_sem.at[week, 0]),
            pltpu.make_async_copy(coupling.at[week], coupling_in.at[week], in_sem.at[week, 1]),
        )

    def order(week):
        blocks = [members[week, k] for k in range(TOUCHED)]
        ranks = [
            sum((blocks[j] < blocks[k]).astype(jnp.int32) for j in range(TOUCHED) if j != k)
            for k in range(TOUCHED)
        ]
        place, sorted_blocks = [], []
        for a in range(TOUCHED):
            here = [(ranks[k] == a).astype(jnp.int32) for k in range(TOUCHED)]
            place.append(sum(here[k] * k for k in range(1, TOUCHED)))
            sorted_blocks.append(sum(here[k] * blocks[k] for k in range(TOUCHED)))
        return place, sorted_blocks

    def prepare(week, slot):
        place, _ = order(week)

        def columns_of(a):
            def work():
                columns = coupling_in[week, :, pl.ds(pl.multiple_of(place[a] * BLOCK, BLOCK), BLOCK)]
                at = slice(a * BLOCK, (a + 1) * BLOCK)
                held[slot][0][:, at], held[slot][1][:, at] = split(columns)
                at = slice(HEAD + a * BLOCK, HEAD + (a + 1) * BLOCK)
                turned[slot][0][at, :], turned[slot][1][at, :] = split(columns.T)

            return work

        def inverse_part(n):
            def work():
                at = slice(n * 128, n * 128 + 128)
                kept[slot][0][at, :], kept[slot][1][at, :] = split(inverse_in[week, at, :])

            return work

        def head():
            row = lax.broadcasted_iota(jnp.int32, (HEAD, LOCAL), 0)
            first = jnp.where(row == 0, jnp.broadcast_to(rhs[pl.ds(week, 1), :], (HEAD, LOCAL)), 0.0)
            turned[slot][0][0:HEAD, :], turned[slot][1][0:HEAD, :] = split(first)

        return [head] + [inverse_part(n) for n in range(4)] + [columns_of(a) for a in range(TOUCHED)]

    def multiply(week, slot):
        _, blocks = order(week)

        def map_part(n, rows):
            def work():
                at = slice(n * 256, n * 256 + 256)
                part = product(
                    (turned[slot][0][rows, :], turned[slot][1][rows, :]),
                    (kept[slot][0][:, at], kept[slot][1][:, at]),
                )
                mapped[0][rows, at], mapped[1][rows, at] = split(part)

            return work

        def add_tiles(n, part, offset, places):
            for b in (2 * n, 2 * n + 1):
                lanes = slice((b - 2 * n) * BLOCK, (b - 2 * n + 1) * BLOCK)
                for a in places:
                    if a == -1:
                        index = 2 * 768 + piece_base(blocks[b]) + (blocks[b] // 8) * 96
                        index += ((blocks[b] // 2) % 4) * 24 + PIECES - 1
                        summed[index] = summed[index] + part[0:8, lanes]
                    elif a <= b:
                        low_half = blocks[a] < 8
                        group = jnp.where(low_half, blocks[a], 15 - blocks[a])
                        piece = jnp.where(low_half, blocks[b] - blocks[a], blocks[b] + 1)
                        first = (piece // PIECES) * 768 + piece % PIECES
                        top = HEAD + a * BLOCK - offset
                        tile = part[top : top + BLOCK, lanes].reshape(16, 8, BLOCK)
                        spots = []
                        for s in range(16):
                            base = first + piece_base(group if s < 8 else 15 - group)
                            spots.append(base + (s % 8 // 4) * 96 + (s % 4) * 24)
                        new = [summed[spots[s]] + tile[s] for s in range(16)]
                        for s in range(16):
                            summed[spots[s]] = new[s]

        def pair_part(n, m):
            def work():
                low = 0 if m == 0 else HEAD + m * 256
                rows = slice(low, HEAD + (m + 1) * 256)
                at = slice(n * 256, n * 256 + 256)
                part = product(
                    (mapped[0][rows, :], mapped[1][rows, :]),
                    (held[slot][0][:, at], held[slot][1][:, at]),
                )
                add_tiles(n, part, low, ([-1] if m == 0 else []) + [2 * m, 2 * m + 1])

            return work

        cuts = [slice(0, HEAD + 256)] + [slice(HEAD + k * 256, HEAD + k * 256 + 256) for k in (1, 2, 3)]
        first = [map_part(n, rows) for rows in cuts for n in range(2)]
        return first + [pair_part(n, m) for n in range(4) for m in range(n + 1)]

    def half_step(week, slot):
        other = 1 - slot

        @pl.when(week + 1 < weeks)
        def arrive():
            for copy in fetch(week + 1):
                copy.wait()

        work = multiply(week, slot)
        more = prepare(jnp.minimum(week + 1, weeks - 1), other)
        for index, item in enumerate(work):
            item()
            if index < len(more):
                more[index]()

    for week in range(2):
        for copy in fetch(week):
            copy.start()

    @pl.loop(0, GRID // 16)
    def clear(index):
        summed[pl.ds(index * 16, 16)] = jnp.zeros((16, 8, BLOCK), f32)

    for copy in fetch(0):
        copy.wait()
    for week in range(2, weeks):
        for copy in fetch(week):
            copy.start()
    for item in prepare(0, 0):
        item()

    @pl.loop(0, weeks // 2)
    def step(index):
        half_step(2 * index, 0)
        half_step(2 * index + 1, 1)


def device(x, y, z, core):
    return {"row": (x // 2) * 8 + z * 2 + core, "col": (x % 2) * 4 + y}


def combine(
    data, matrix, rhs, prior, weight,
    out_matrix, out_rhs, out_solution,
    own, other, relay1, final1, sum1, relay2, final2, sum2, final3, sum3,
    land, block_out, blocks_in, partial1, partial2, row1, column1, row2,
    pair_send, pair_recv, ring_send, ring_recv,
    tile_send, tile_recv, block_send, block_recv,
    one_send, one_recv, column_send, column_recv, two_send, two_recv,
):
    r, c = lax.axis_index("row"), lax.axis_index("col")
    core, z = r % 2, (r // 2) % 4
    x, y = (r // 8) * 2 + c // 4, c % 4
    me = (x, y, z)

    def neighbour(axis, step):
        at = list(me)
        at[axis] = (me[axis] + step) % 4
        return device(*at, core)

    barrier = pltpu.get_barrier_semaphore()
    partner = {"row": r + 1 - 2 * core, "col": c}
    greeted = [partner] + [neighbour(axis, step) for axis in range(3) for step in (1, 3)]
    for target in greeted:
        pl.semaphore_signal(barrier, inc=1, device_id=target, device_id_type=MESH)

    strip_rows = [pl.ds(24 * part, 24) for part in range(2)]

    def cut(ref, lead, dims, position, index, part, half=None):
        picks = [slice(None)] * dims
        picks[position] = index
        if half is not None:
            picks[0 if position else 1] = pl.ds(2 * half, 2)
        return ref.at[(*lead, *picks, strip_rows[part])]

    def pairs(color, j, part):
        at = (me[color] + j) % 4
        return pltpu.make_async_remote_copy(
            src_ref=cut(data, (color, 1 - core), 3, color, at, part),
            dst_ref=cut(other, (color,), 3, color, at, part),
            send_sem=pair_send.at[part, color, j],
            recv_sem=pair_recv.at[part, color, j],
            device_id=partner,
            device_id_type=MESH,
        )

    everything = [(2, 0), (1, 0), (3, 0), (2, 1), (0, 0), (1, 1), (3, 1), (0, 1)]
    pl.semaphore_wait(barrier, len(greeted))
    for j, part in everything:
        for color in range(COLORS):
            pairs(color, j, part).start()

    def add(target, *terms):
        value = target[...]
        for term in terms:
            value = value + term[...]
        target[...] = value

    def arrived(color, j, part):
        at = (me[color] + j) % 4
        pairs(color, j, part).wait_recv()
        mine = cut(data, (color, core), 3, color, at, part)
        total = mine[...] + cut(other, (color,), 3, color, at, part)[...]
        cut(own, (color,), 3, color, at, part)[...] = total

    axes = ((0, 1, 2), (1, 2, 0), (2, 0, 1))
    spots = ((0, 0), (1, 1), (2, 0))
    waiting = []

    def hop(number, color, slot, step, part, src, dst):
        return pltpu.make_async_remote_copy(
            src_ref=src,
            dst_ref=dst,
            send_sem=ring_send.at[part, number, color, slot],
            recv_sem=ring_recv.at[part, number, color, slot],
            device_id=neighbour(axes[color][number], step),
            device_id_type=MESH,
        )

    def ring(number, source, relay, final, result, prepare):
        dims = 3 - number

        def source_cut(color, step, part, half=None):
            at = (me[axes[color][number]] + step) % 4
            return cut(source, (color,), dims, spots[color][number], at, part, half)

        def landing(color, side, part, half=None):
            picks = [slice(None)] * (dims - 1)
            if half is not None:
                picks[0] = pl.ds(2 * half, 2)
            return final.at[(color, side, *picks, strip_rows[part])]

        def relayed(color, side, part):
            return relay.at[(color, side, *[slice(None)] * (dims - 1), strip_rows[part])]

        def away(color, side, part):
            src = source_cut(color, 2, part, side)
            return hop(number, color, side, (1, 3)[side], part, src, relayed(color, side, part))

        def near(color, side, part, half):
            step = (1, 3)[side]
            src = source_cut(color, step, part, half)
            dst = landing(color, side, part, half)
            return hop(number, color, 2 + 2 * side + half, step, part, src, dst)

        def far(part):
            for color in range(COLORS):
                prepare(color, 2, part)
                for side in range(2):
                    away(color, side, part).start()
                    waiting.append(away(color, side, part))

        def close(part):
            for color in range(COLORS):
                for side in range(2):
                    prepare(color, (1, 3)[side], part)
                    near(color, side, part, 1 - side).start()

        def pass_on(part):
            for color in range(COLORS):
                for side in range(2):
                    away(color, side, part).wait_recv()
                    add(source_cut(color, (1, 3)[side], part, side), relayed(color, side, part))
                    near(color, side, part, side).start()

        def finish(part):
            for color in range(COLORS):
                prepare(color, 0, part)
                for side in range(2):
                    for half in range(2):
                        near(color, side, part, half).wait_recv()
                        waiting.append(near(color, side, part, half))
                total = source_cut(color, 0, part)[...] + landing(color, 0, part)[...]
                picks = [slice(None)] * (dims - 1)
                result[(color, *picks, strip_rows[part])] = total + landing(color, 1, part)[...]

        return far, close, pass_on, finish

    def nothing(color, j, part):
        pass

    def direct(color, step, part):
        at = (me[axes[color][2]] + step) % 4
        src = sum2.at[color, at, strip_rows[part]]
        return hop(2, color, step - 1, step, part, src, final3.at[color, step - 1, strip_rows[part]])

    def last_out(part):
        for step in (2, 1, 3):
            for color in range(COLORS):
                direct(color, step, part).start()
                waiting.append(direct(color, step, part))

    def last_in(part):
        for color in range(COLORS):
            total = sum2[color, me[axes[color][2]], strip_rows[part]]
            for step in (1, 3, 2):
                direct(color, step, part).wait_recv()
                total = total + final3[color, step - 1, strip_rows[part]]
            sum3[color, strip_rows[part]] = total

    far1, close1, pass1, finish1 = ring(0, own, relay1, final1, sum1, arrived)
    far2, close2, pass2, finish2 = ring(1, sum1, relay2, final2, sum2, nothing)
    far1(0), close1(0), far1(1), pass1(0), close1(1), finish1(0)
    far2(0), close2(0), pass1(1), pass2(0), finish1(1)
    far2(1), close2(1), finish2(0), last_out(0), pass2(1), last_in(0)
    finish2(1), last_out(1), last_in(1)

    low_half = r < 8
    group = jnp.where(low_half, r, 15 - r)
    strip = jnp.where(low_half, c, c + 8)

    def piece(t):
        return sum3.at[t // PIECES, pl.ds((t % PIECES) * 8, 8)]

    def tile_copy(t, mirrored):
        first = t < 16 - group
        i = jnp.where(first, group, 15 - group)
        j = jnp.where(first, group + t, t - 1)
        row, column = (j, i) if mirrored else (i, j)
        copy = pltpu.make_async_remote_copy(
            src_ref=piece(t),
            dst_ref=land.at[column % 2, strip],
            send_sem=tile_send.at[t, int(mirrored)],
            recv_sem=tile_recv.at[column % 2, strip],
            device_id={"row": row, "col": column // 2},
            device_id_type=MESH,
        )
        mine = (row == r) & (column // 2 == c)
        wanted = (i != j) if mirrored else None
        return copy, mine, wanted, column % 2

    holder = c == r // 2

    def to_column(d):
        return pltpu.make_async_remote_copy(
            src_ref=block_out,
            dst_ref=blocks_in.at[1 + r % 2],
            send_sem=block_send.at[d],
            recv_sem=block_recv.at[1 + r % 2],
            device_id={"row": (r + d) % 16, "col": c},
            device_id_type=MESH,
        )

    def to_row(d):
        return pltpu.make_async_remote_copy(
            src_ref=block_out,
            dst_ref=blocks_in.at[0],
            send_sem=block_send.at[15 + d],
            recv_sem=block_recv.at[0],
            device_id={"row": r, "col": (c + d) % 8},
            device_id_type=MESH,
        )

    for t in range(17):
        for mirrored in (False, True):
            copy, mine, wanted, side = tile_copy(t, mirrored)
            away = jnp.logical_not(mine)
            if wanted is not None:
                mine, away = mine & wanted, away & wanted

            @pl.when(away)
            def send():
                copy.start()

            @pl.when(mine)
            def keep():
                land[side, strip] = piece(t)[...]

    @pl.when(holder)
    def hand_out():
        reduced = rhs[...] - sum3[2, 40:41, :]
        row = lax.broadcasted_iota(jnp.int32, (8, BLOCK), 0)
        value = jnp.where(row == 0, reduced, jnp.where(row == 1, prior[...], weight[...]))
        block_out[...] = value
        blocks_in[0] = value
        blocks_in[1 + r % 2] = value
        for d in range(1, 16):
            to_column(d).start()
        for d in range(1, 8):
            to_row(d).start()

    def receive(buffer, semaphore):
        pltpu.make_async_remote_copy(
            src_ref=buffer,
            dst_ref=buffer,
            send_sem=semaphore,
            recv_sem=semaphore,
            device_id=partner,
            device_id_type=MESH,
        ).wait_recv()

    for side in range(2):
        column = 2 * c + side
        low = jnp.minimum(r, column)
        owner = jnp.where(low < 8, low, 15 - low)
        for s in range(16):
            row = owner if s < 8 else 15 - owner

            @pl.when(jnp.logical_not((row == r) & (c == s % 8)))
            def wait():
                receive(land.at[side, s], tile_recv.at[side, s])

    tiles = []
    for side in range(2):
        found = land[side].reshape(BLOCK, BLOCK)
        found = jnp.where(r > 2 * c + side, found.T, found)
        lanes = slice(side * BLOCK, (side + 1) * BLOCK)
        tile = matrix[:, lanes] - found
        out_matrix[:, lanes] = tile
        tiles.append(tile)

    @pl.when(jnp.logical_not(holder))
    def row_block():
        receive(blocks_in.at[0], block_recv.at[0])

    for side in range(2):

        @pl.when(r != 2 * c + side)
        def column_block():
            receive(blocks_in.at[1 + side], block_recv.at[1 + side])

    reduced = blocks_in[0, 0:1, :]
    out_rhs[...] = reduced

    def matvec(first, second):
        spread = tiles[0] * first + tiles[1] * second
        return jnp.broadcast_to(jnp.sum(spread.T, axis=0, keepdims=True), (8, BLOCK))

    def along_row(d, source, target, sends, recvs):
        return pltpu.make_async_remote_copy(
            src_ref=source,
            dst_ref=target.at[c],
            send_sem=sends.at[d],
            recv_sem=recvs.at[c],
            device_id={"row": r, "col": (c + d) % 8},
            device_id_type=MESH,
        )

    def along_column(d):
        return pltpu.make_async_remote_copy(
            src_ref=partial1,
            dst_ref=column1.at[r % 2, c],
            send_sem=column_send.at[d],
            recv_sem=column_recv.at[r % 2, c],
            device_id={"row": (r + d) % 16, "col": r // 2},
            device_id_type=MESH,
        )

    value = matvec(blocks_in[1, 1:2, :], blocks_in[2, 1:2, :])
    partial1[...] = value
    row1[c] = value
    for d in range(1, 16):
        along_column(d).start()

    @pl.when(jnp.logical_not(holder))
    def last_column():
        along_column(0).start()

    @pl.when(holder)
    def own_column():
        column1[r % 2, c] = value

    for d in range(1, 8):
        along_row(d, partial1, row1, one_send, one_recv).start()

    def gather_row(target, recvs):
        for s in range(8):

            @pl.when(c != s)
            def wait():
                receive(target.at[s], recvs.at[s])

    def total(ref):
        value = ref[0, 0:1, :]
        for s in range(1, 8):
            value = value + ref[s, 0:1, :]
        return value

    def updated(block, product):
        return block[1:2, :] + block[2:3, :] * (block[0:1, :] - product)

    for side in range(2):
        for s in range(8):

            @pl.when(jnp.logical_not((r == 2 * c + side) & (c == s)))
            def wait():
                receive(column1.at[side, s], column_recv.at[side, s])

    first = [updated(blocks_in[1 + side], total(column1.at[side])) for side in range(2)]
    value = matvec(*first)
    partial2[...] = value
    row2[c] = value
    for d in range(1, 8):
        along_row(d, partial2, row2, two_send, two_recv).start()
    gather_row(row1, one_recv)
    mine = updated(blocks_in[0], total(row1))
    gather_row(row2, two_recv)
    out_solution[...] = mine + weight[...] * (reduced - total(row2))

    for j, part in everything:
        for color in range(COLORS):
            pairs(color, j, part).wait_send()
    for copy in waiting:
        copy.wait_send()
    for t in range(17):
        for mirrored in (False, True):
            copy, mine, wanted, side = tile_copy(t, mirrored)
            away = jnp.logical_not(mine)
            if wanted is not None:
                away = away & wanted

            @pl.when(away)
            def sent():
                copy.wait_send()

    @pl.when(holder)
    def handed():
        for d in range(1, 16):
            to_column(d).wait_send()
        for d in range(1, 8):
            to_row(d).wait_send()

    for d in range(1, 16):
        along_column(d).wait_send()

    @pl.when(jnp.logical_not(holder))
    def last_sent():
        along_column(0).wait_send()

    for d in range(1, 8):
        along_row(d, partial1, row1, one_send, one_recv).wait_send()
        along_row(d, partial2, row2, two_send, two_recv).wait_send()


def partial_sum(local_inverse, coupling, local_rhs, members):
    local_inverse = pltpu.with_memory_space_constraint(local_inverse, pltpu.HBM)
    coupling = pltpu.with_memory_space_constraint(coupling, pltpu.HBM)
    members = pltpu.with_memory_space_constraint(members, pltpu.HBM)
    local_rhs = pltpu.with_memory_space_constraint(local_rhs, pltpu.HBM)

    def two(rows, columns, dtype=bf16):
        return (pltpu.VMEM((rows, columns), dtype),) * 2

    weeks, columns = local_inverse.shape[0], TOUCHED * BLOCK
    return pl.pallas_call(
        eliminate,
        grid_spec=pltpu.PrefetchScalarGridSpec(
            num_scalar_prefetch=1,
            grid=(1,),
            in_specs=[
                pl.BlockSpec(memory_space=pl.ANY),
                pl.BlockSpec(memory_space=pl.ANY),
                pl.BlockSpec(local_rhs.shape, lambda step, m: (0, 0)),
            ],
            out_specs=pl.BlockSpec(memory_space=pltpu.VMEM),
            scratch_shapes=[
                pltpu.VMEM((weeks, LOCAL, LOCAL), f32),
                pltpu.VMEM((weeks, LOCAL, columns), f32),
                pltpu.SemaphoreType.DMA((weeks, 2)),
                (two(HEAD + columns, LOCAL),) * 2,
                (two(LOCAL, columns),) * 2,
                (two(LOCAL, LOCAL),) * 2,
                two(HEAD + columns, LOCAL),
            ],
        ),
        out_shape=jax.ShapeDtypeStruct((GRID, 8, BLOCK), f32),
        compiler_params=pltpu.CompilerParams(
            vmem_limit_bytes=42 * 2**20
        ),
        name="eliminate",
    )(members, local_inverse, coupling, local_rhs)


def combined(summed, shared_matrix, shared_rhs, prior_solution, preconditioner):
    rows, columns = shared_matrix.shape
    vmem = pl.BlockSpec(memory_space=pltpu.VMEM)
    strip = PIECES * 8
    dma = pltpu.SemaphoreType.DMA

    def buffer(*shape):
        return pltpu.VMEM(shape, f32)

    return pl.pallas_call(
        combine,
        in_specs=[vmem] * 5,
        out_specs=[vmem] * 3,
        out_shape=[
            jax.ShapeDtypeStruct((rows, columns), f32),
            jax.ShapeDtypeStruct((1, rows), f32),
            jax.ShapeDtypeStruct((1, rows), f32),
        ],
        scratch_shapes=[
            buffer(COLORS, 4, 4, 4, strip, BLOCK),
            buffer(COLORS, 4, 4, 4, strip, BLOCK),
            buffer(COLORS, 2, 2, 4, strip, BLOCK),
            buffer(COLORS, 2, 4, 4, strip, BLOCK),
            buffer(COLORS, 4, 4, strip, BLOCK),
            buffer(COLORS, 2, 2, strip, BLOCK),
            buffer(COLORS, 2, 4, strip, BLOCK),
            buffer(COLORS, 4, strip, BLOCK),
            buffer(COLORS, 3, strip, BLOCK),
            buffer(COLORS, strip, BLOCK),
            buffer(2, 16, 8, BLOCK),
            buffer(8, BLOCK),
            buffer(3, 8, BLOCK),
            buffer(8, BLOCK),
            buffer(8, BLOCK),
            buffer(8, 8, BLOCK),
            buffer(2, 8, 8, BLOCK),
            buffer(8, 8, BLOCK),
            dma((2, COLORS, 4)),
            dma((2, COLORS, 4)),
            dma((2, 3, COLORS, 6)),
            dma((2, 3, COLORS, 6)),
            dma((17, 2)),
            dma((2, 16)),
            dma((23,)),
            dma((3,)),
            dma((8,)),
            dma((8,)),
            dma((16,)),
            dma((2, 8)),
            dma((8,)),
            dma((8,)),
        ],
        compiler_params=pltpu.CompilerParams(
            collective_id=0, has_side_effects=True, vmem_limit_bytes=24 * 2**20
        ),
        name="combine",
    )(
        summed.reshape(COLORS, 2, 4, 4, 4, strip, BLOCK),
        shared_matrix,
        shared_rhs.reshape(1, rows),
        prior_solution.reshape(1, rows),
        preconditioner.reshape(1, rows),
    )


def local(
    local_inverse,
    coupling,
    local_rhs,
    members,
    shared_matrix,
    shared_rhs,
    prior_solution,
    preconditioner,
):
    summed = partial_sum(local_inverse, coupling, local_rhs, members)
    reduced_matrix, reduced_rhs, solution = combined(
        summed, shared_matrix, shared_rhs, prior_solution, preconditioner
    )
    return reduced_matrix, reduced_rhs.reshape(-1), solution.reshape(-1)


def solution(mesh):
    both = ("row", "col")
    placed = (
        P(both, None, None),
        P(both, None, None),
        P(both, None),
        P(both, None),
        P("row", "col"),
        P("row"),
        P("row"),
        P("row"),
    )
    return jax.shard_map(
        local,
        mesh=mesh,
        in_specs=placed,
        out_specs=(P("row", "col"), P("row"), P("row")),
        check_vma=False,
    )
```
